128 devices in a mesh: grp: 4 (over x_hi, core), dev: 32 (over y, x_lo, z).
Axes of the slice: x: 4 (x_hi: 2, x_lo: 2; x = x_hi * 2 + x_lo), y: 4, z: 4, core: 2. Of those that a mesh axis runs over, the one named last changes fastest.
Arguments:
- coefficients: float32 [2, 8, 64, 16384], P(None, None, None, ('grp', 'dev')), may hold values from -6 to 6
- spatial_root: int32 [256], replicated, may hold values from 0 to 1023
- frequency_root: int32 [256], replicated, may hold values from 0 to 255
Outputs:
- result: float32 [2, 8, 64, 16384], P(None, None, None, ('grp', 'dev'))
The draws below stay inside these ranges and needn't reach their ends.
All inputs are finite; a program needn't handle non-finite values.
Results may differ from the reference program's by a relative error of at most 0.002.
Values sent between devices are 32-bit elements; how exact they have to be, the bound alone decides.
No kernel may reach another device: no remote copies, remote signals or barrier semaphores. Data moves between devices by JAX's collectives and lax.ppermute only.
A program may use at most 64 MiB of HBM per device.

```python
import math
import jax
import jax.numpy as jnp
from jax import lax

R = 64
S = 8
LEVELS = 12
PD = 128
NB = 256
PAIRS = 16384
N_DEV = 32


def touch_ends(array, own_key, smallest, high):
    place = [jax.random.randint(jax.random.fold_in(own_key, axis), (), 0, length) for axis, length in enumerate(array.shape)]
    longest = array.shape.index(max(array.shape))
    neighbour = place[:longest] + [(place[longest] + 1) % array.shape[longest]] + place[longest + 1:]
    return array.at[tuple(place)].set(smallest).at[tuple(neighbour)].set(high)


def block_levels(stream_key, shape, shards, smallest, top_value):
    factor_of, own = 1.0, jax.random.fold_in(stream_key, 6)
    for dim, blocks in shards:
        draws = jnp.exp(jax.random.uniform(jax.random.fold_in(own, dim), (blocks,), jnp.float32, smallest / len(shards), top_value / len(shards)))
        factor_of = factor_of * jnp.repeat(draws, shape[dim] // blocks).reshape([-1 if axis == dim else 1 for axis in range(len(shape))])
    return factor_of


def noise(stream_key, dims, deviation, bound, pieces=(), kind=jnp.bfloat16):
    level = block_levels(stream_key, dims, pieces, -0.22, 0.18) if pieces else 1.0
    entries = jax.random.normal(stream_key, dims, jnp.float32) * deviation * level
    return jnp.minimum(jnp.maximum(entries, -bound), bound).astype(kind)


def setup_inputs(seed: int = 0) -> dict:
    keys = jax.random.split(jax.random.key(seed), 4)
    coefficients = noise(keys[0], (2, S, R, PAIRS), 1.0, 6.0, ((3, 128),), jnp.float32)
    spatial_root = touch_ends(jax.random.randint(keys[1], (NB,), 0, 4 ** (LEVELS // 2 - 1)), jax.random.fold_in(keys[1], 1), 0, (4 ** (LEVELS // 2 - 1)) - 1).astype(jnp.int32)
    frequency_root = touch_ends(jax.random.randint(keys[2], (NB,), 0, 4 ** (LEVELS // 2 - 2)), jax.random.fold_in(keys[2], 1), 0, (4 ** (LEVELS // 2 - 2)) - 1).astype(jnp.int32)
    return {"coefficients": coefficients, "spatial_root": spatial_root, "frequency_root": frequency_root}


HIGHEST = lax.Precision.HIGHEST

def cheb_nodes():
    node_order = jnp.arange(8, dtype=jnp.float32)
    return 0.5 - 0.5 * jnp.cos(math.pi * (2.0 * node_order + 1.0) / 16.0)

def lagrange_table(half_cell):
    points = cheb_nodes()
    target = (points + half_cell) / 2.0
    diagonal = jnp.arange(8)[:, None] == jnp.arange(8)[None, :]
    numerator = jnp.where(diagonal[None, :, :], jnp.float32(1.0), target[:, None, None] - points[None, None, :])
    denominator = jnp.where(diagonal, jnp.float32(1.0), points[:, None] - points[None, :])
    return jnp.prod(numerator, axis=2) / jnp.prod(denominator, axis=1)[None, :]

def interp_tables():
    halves = [lagrange_table(0.0), lagrange_table(1.0)]
    return jnp.stack([jnp.kron(halves[quadrant % 2], halves[quadrant // 2]) for quadrant in range(4)])

def pair_digits(pair_index, pairs_dev, devices_dev):
    quarter = pairs_dev // 4
    within = pair_index % pairs_dev
    device = pair_index // pairs_dev % devices_dev
    group_id = pair_index // (pairs_dev * devices_dev)
    places = [device % 4, group_id % 4, within // quarter]
    return (places, device // 4 * quarter + within % quarter)

def pair_boxes(pair_index, level_step, box_roots, pairs_dev, devices_dev, levels):
    places, _ = pair_digits(pair_index, pairs_dev, devices_dev)
    coarse_space = levels // 2 - 1
    coarse_wave = levels // 2 - 2
    space_row = box_roots[0] // 2 ** coarse_space
    space_column = box_roots[0] % 2 ** coarse_space
    for position in range(level_step):
        space_row = 2 * space_row + places[position] % 2
        space_column = 2 * space_column + places[position] // 2
    wave_row = box_roots[1] // 2 ** coarse_wave
    wave_column = box_roots[1] % 2 ** coarse_wave
    for position in range(2, level_step - 1, -1):
        wave_row = 2 * wave_row + places[position] % 2
        wave_column = 2 * wave_column + places[position] // 2
    space_side = 0.5 ** (coarse_space + level_step)
    wave_side = float(2 ** levels) / float(2 ** (coarse_wave + 3 - level_step))
    offset = -0.5 * float(2 ** levels)
    space_box = (space_row.astype(jnp.float32) * space_side, space_column.astype(jnp.float32) * space_side, space_side)
    wave_box = (offset + wave_row.astype(jnp.float32) * wave_side, offset + wave_column.astype(jnp.float32) * wave_side, wave_side)
    return (space_box, wave_box)

def box_points(square):
    points = cheb_nodes()
    first_axis = jnp.repeat(points, 8)
    second_axis = jnp.tile(points, 8)
    return (square[0][None, :] + square[2] * first_axis[:, None], square[1][None, :] + square[2] * second_axis[:, None])

def box_center(square):
    return (square[0] + 0.5 * square[2], square[1] + 0.5 * square[2])

def phase_angle(first_space, second_space, first_wave, second_wave):
    two_pi = 2.0 * math.pi
    wave_speed = 16.0 * math.pi
    speed_one = (2.0 + jnp.sin(wave_speed * first_space) * jnp.sin(wave_speed * second_space)) / 16.0
    speed_two = (2.0 + jnp.cos(wave_speed * first_space) * jnp.cos(wave_speed * second_space)) / 16.0
    radial = jnp.sqrt(speed_one * speed_one * first_wave * first_wave + speed_two * speed_two * second_wave * second_wave)
    return two_pi * (first_space * first_wave + second_space * second_wave + radial)

def rotate(values, turn_angle):
    cosine = jnp.cos(turn_angle)
    sine_part = jnp.sin(turn_angle)
    return jnp.stack([values[0] * cosine - values[1] * sine_part, values[0] * sine_part + values[1] * cosine])

def pre_merge(children, new_index, new_roots, child_index, child_roots, pairs_dev, devices_dev, levels):
    space_box, wave_box = pair_boxes(new_index, 1, new_roots, pairs_dev, devices_dev, levels)
    center_one, center_two = box_center(space_box)
    turned = []
    for child_id in range(4):
        _, child_wave = pair_boxes(child_index[child_id], 0, (child_roots[0][child_id], child_roots[1][child_id]), pairs_dev, devices_dev, levels)
        wave_one, wave_two = box_points(child_wave)
        turned.append(rotate(children[child_id], -phase_angle(center_one[None, :], center_two[None, :], wave_one, wave_two)))
    summed = jnp.einsum('cst,caksm->aktm', interp_tables(), jnp.stack(turned), precision=HIGHEST)
    wave_one, wave_two = box_points(wave_box)
    return rotate(summed, phase_angle(center_one[None, :], center_two[None, :], wave_one, wave_two))

def switch_step(values, pair_index, box_roots, pairs_dev, devices_dev, levels):
    space_box, wave_box = pair_boxes(pair_index, 1, box_roots, pairs_dev, devices_dev, levels)
    space_one, space_two = box_points(space_box)
    wave_one, wave_two = box_points(wave_box)
    kernel_angle = phase_angle(space_one[:, None, :], space_two[:, None, :], wave_one[None, :, :], wave_two[None, :, :])
    cosine = jnp.cos(kernel_angle)
    sine_part = jnp.sin(kernel_angle)
    real_part = jnp.einsum('tsm,ksm->ktm', cosine, values[0], precision=HIGHEST) - jnp.einsum('tsm,ksm->ktm', sine_part, values[1], precision=HIGHEST)
    imag_part = jnp.einsum('tsm,ksm->ktm', sine_part, values[0], precision=HIGHEST) + jnp.einsum('tsm,ksm->ktm', cosine, values[1], precision=HIGHEST)
    return jnp.stack([real_part, imag_part]) / 64.0

def post_terms(values, pair_index, box_roots, level_step, pairs_dev, devices_dev, levels):
    space_box, wave_box = pair_boxes(pair_index, level_step, box_roots, pairs_dev, devices_dev, levels)
    space_one, space_two = box_points(space_box)
    center_one, center_two = box_center(wave_box)
    return rotate(values, -phase_angle(space_one, space_two, center_one[None, :], center_two[None, :]))

def post_finish(merged, pair_index, box_roots, level_step, pairs_dev, devices_dev, levels):
    space_box, wave_box = pair_boxes(pair_index, level_step, box_roots, pairs_dev, devices_dev, levels)
    space_one, space_two = box_points(space_box)
    center_one, center_two = box_center(wave_box)
    return rotate(merged, phase_angle(space_one, space_two, center_one[None, :], center_two[None, :]))

def lookup_roots(pair_index, spatial_root, frequency_root):
    _, block_id = pair_digits(pair_index, PD, N_DEV)
    return (jnp.take(spatial_root, block_id), jnp.take(frequency_root, block_id))

def reference(coefficients, spatial_root, frequency_root):
    rhs_count = coefficients.shape[1]
    rank_count = coefficients.shape[2]
    pairs = coefficients.shape[3]
    pair_index = jnp.arange(pairs, dtype=jnp.int32)
    box_roots = lookup_roots(pair_index, spatial_root, frequency_root)
    outer_count = pairs // (4 * PD)
    children = jnp.moveaxis(coefficients.reshape(2, rhs_count, rank_count, outer_count, 4, PD), 4, 0).reshape(4, 2, rhs_count, rank_count, outer_count * PD)
    child_index = jnp.moveaxis(pair_index.reshape(outer_count, 4, PD), 1, 0).reshape(4, outer_count * PD)
    child_roots = (jnp.moveaxis(box_roots[0].reshape(outer_count, 4, PD), 1, 0).reshape(4, outer_count * PD), jnp.moveaxis(box_roots[1].reshape(outer_count, 4, PD), 1, 0).reshape(4, outer_count * PD))
    merged = []
    for quadrant in range(4):
        outcome = pre_merge(children, child_index[quadrant], (child_roots[0][quadrant], child_roots[1][quadrant]), child_index, child_roots, PD, N_DEV, LEVELS)
        merged.append(outcome.reshape(2, rhs_count, rank_count, outer_count, PD))
    first_level = jnp.stack(merged, axis=4).reshape(2, rhs_count, rank_count, pairs)
    blocks = pairs // PD

    def switch_block(packed):
        return switch_step(packed[0], packed[1], (packed[2], packed[3]), PD, N_DEV, LEVELS)
    switched = lax.map(switch_block, (jnp.moveaxis(first_level.reshape(2, rhs_count, rank_count, blocks, PD), 3, 0), pair_index.reshape(blocks, PD), box_roots[0].reshape(blocks, PD), box_roots[1].reshape(blocks, PD)))
    switched = jnp.moveaxis(switched, 0, 3).reshape(2, rhs_count, rank_count, pairs)
    child_terms = post_terms(switched, pair_index, box_roots, 1, PD, N_DEV, LEVELS)
    summed = lax.optimization_barrier(jnp.sum(child_terms.reshape(2, rhs_count, rank_count, 4, pairs // 4), axis=3))
    spread = jnp.einsum('jts,aksm->aktjm', interp_tables(), summed, precision=HIGHEST).reshape(2, rhs_count, rank_count, pairs)
    second = post_finish(spread, pair_index, box_roots, 2, PD, N_DEV, LEVELS)
    child_terms = post_terms(second, pair_index, box_roots, 2, PD, N_DEV, LEVELS)
    summed = lax.optimization_barrier(jnp.sum(child_terms.reshape(2, rhs_count, rank_count, outer_count * 4, 4, PD // 4), axis=4))
    spread = jnp.einsum('jts,aksgm->aktgjm', interp_tables(), summed, precision=HIGHEST).reshape(2, rhs_count, rank_count, pairs)
    return post_finish(spread, pair_index, box_roots, 3, PD, N_DEV, LEVELS)
```

```python
import functools

import jax
import jax.numpy as jnp
import numpy as np
from jax import lax
from jax.experimental import pallas as pl
from jax.experimental.pallas import tpu as pltpu
from jax.sharding import PartitionSpec as P


F32 = jnp.float32
BF16 = jnp.bfloat16
VMEM = pl.BlockSpec(memory_space=pltpu.VMEM)
SMEM = pl.BlockSpec(memory_space=pltpu.SMEM)

COS = (0.99999922, -19.73898252, 64.92872662, -85.27239701, 58.79403871, -21.07678212)
SIN = (6.28318282, -41.3414214, 81.59618388, -76.58010057, 41.20539503, -12.27126259)

NODES = 0.5 - 0.5 * np.cos(np.pi * (2.0 * np.arange(8) + 1.0) / 16.0)
Z = [float(node) for node in NODES]


def lagrange_table(half_cell):
    target = (NODES + half_cell) / 2.0
    table = np.ones((8, 8))
    for s in range(8):
        for n in range(8):
            if n != s:
                table[:, s] *= (target - NODES[n]) / (NODES[s] - NODES[n])
    return table


HALVES = [lagrange_table(0.0), lagrange_table(1.0)]
V = [np.kron(HALVES[u % 2], HALVES[u // 2]) for u in range(4)]
MERGE = np.concatenate([table.T for table in V], axis=1)
SPREAD = np.stack([np.concatenate([V[u2] @ V[u1] for u2 in range(4)]) for u1 in range(4)])


def in_two(table):
    high = jnp.asarray(table, F32).astype(BF16)
    low = (jnp.asarray(table, F32) - high.astype(F32)).astype(BF16)
    return high, low


def polynomial(square, terms, scale):
    value = jnp.full_like(square, terms[-1] * scale)
    for term in terms[-2::-1]:
        value = value * square + term * scale
    return value


def fraction(turns):
    return turns - jnp.round(turns)


def cos_sin(turns, scale=1.0):
    part = fraction(turns)
    square = part * part
    return polynomial(square, COS, scale), part * polynomial(square, SIN, scale)


def root(value):
    return value * lax.rsqrt(value)


def speeds(first_cos_sin, second_cos_sin):
    one = (2.0 + first_cos_sin[1] * second_cos_sin[1]) * (1.0 / 16.0)
    two = (2.0 + first_cos_sin[0] * second_cos_sin[0]) * (1.0 / 16.0)
    return one * one, two * two


def lanes():
    return lax.broadcasted_iota(jnp.int32, (8, 128), 1)


def by_sublane(values):
    row = lax.broadcasted_iota(jnp.int32, (8, 128), 0)
    out = jnp.full((8, 128), values[0], F32)
    for index in range(1, 8):
        out = jnp.where(row == index, values[index], out)
    return out


def from_scalars(ref, base, period):
    place = lanes() % period
    out = jnp.full((8, 128), ref[base], jnp.int32)
    for index in range(1, period):
        out = jnp.where(place == index, ref[base + index], out)
    return out


def swap_digit(parts, bits, first_lane):
    lane = lax.broadcasted_iota(jnp.int32, parts[0].shape, parts[0].ndim - 1)
    parts = list(parts)
    for bit in range(bits):
        step = 1 << bit
        shift = first_lane << bit
        low = lane // shift % 2 == 0
        for index in range(len(parts)):
            if index & step:
                continue
            a, b = parts[index], parts[index | step]
            axis = a.ndim - 1
            parts[index] = jnp.where(low, a, pltpu.roll(b, shift, axis))
            parts[index | step] = jnp.where(low, pltpu.roll(a, 128 - shift, axis), b)
    return parts


def pack_kernel(x_ref, out0, out1, out2, out3, held):
    z = lax.axis_index("dev") % 4
    for part in range(2):
        for low in range(2):
            for tile in range(8):
                rows = pl.ds(8 * tile, 8)
                group = [x_ref[part, 2 * high + low, rows, :] for high in range(4)]
                for target, value in enumerate(swap_digit(group, 2, 8)):
                    held[target, part, low, rows, :] = value
    for distance, out in enumerate((out0, out1, out2, out3)):
        target = (z + distance) % 4
        out[...] = held[target]


def table_kernel(space_ref, wave_ref, ec, es, k_cos, k_dif, k_sum, rc, rs, first, second, left, right):
    group = lax.axis_index("grp")
    device = lax.axis_index("dev")
    z = device % 4
    base = device // 4 * 32
    lane = lanes()
    node = by_sublane(Z)
    u1x, u1y = group % 2, group // 2
    u2 = lane // 32
    u2x, u2y = u2 % 2, u2 // 2

    space = from_scalars(space_ref, base + z * 8, 8)
    wave = from_scalars(wave_ref, base + z * 8, 8)
    space_x, space_y = space // 32, space % 32
    wave_x, wave_y = wave // 16, wave % 16

    for u0 in range(4):
        ix, iy = 2 * space_x + u0 % 2, 2 * space_y + u0 // 2
        fx, fy = ix.astype(F32) + 0.5, iy.astype(F32) + 0.5
        one, two = speeds(cos_sin(fx * 0.125), cos_sin(fy * 0.125))
        for c in range(4):
            kx = wave_x * 8 + u2x * 4 + u1x * 2 + c % 2 - 64
            ky = wave_y * 8 + u2y * 4 + u1y * 2 + c // 2 - 64
            whole = (((2 * ix + 1) * kx + (2 * iy + 1) * ky) & 3).astype(F32) * 0.25
            fkx, fky = kx.astype(F32), ky.astype(F32)
            k2 = (fky + node) * 32.0
            part2 = whole + fy * 0.5 * node
            rad2 = two * (k2 * k2)
            for s1 in range(8):
                k1 = (fkx + Z[s1]) * 32.0
                turns = part2 + fx * (0.5 * Z[s1]) + root(one * (k1 * k1) + rad2)
                cosine, sine = cos_sin(turns)
                ec[u0, c, pl.ds(8 * s1, 8), :] = cosine
                es[u0, c, pl.ds(8 * s1, 8), :] = -sine

    u0 = lane // 8 % 4
    ix, iy = 2 * space_x + u0 % 2, 2 * space_y + u0 // 2
    kx, ky = wave_x * 4 + u2x * 2 + u1x - 32, wave_y * 4 + u2y * 2 + u1y - 32
    fx, fy = ix.astype(F32), iy.astype(F32)
    fkx, fky = kx.astype(F32), ky.astype(F32)
    half_x = ((kx + ix) & 1).astype(F32) * 0.5
    half_y = ((ky + iy) & 1).astype(F32) * 0.5
    one_a, two_a = speeds(cos_sin((fx + 0.5) * 0.125), cos_sin((fy + 0.5) * 0.125))
    turn2 = cos_sin((fy + node) * 0.125)
    squares1, squares2 = [], []
    for s in range(8):
        k1, k2 = (fkx + Z[s]) * 64.0, (fky + Z[s]) * 64.0
        squares1.append(k1 * k1)
        squares2.append(k2 * k2)
    for s1 in range(8):
        for s2 in range(8):
            linear = (2.0 * fy + 0.5) * Z[s2] + node * (Z[s2] - 0.5) + half_y
            right[s1, s2] = fraction(linear + root(one_a * squares1[s1] + two_a * squares2[s2]))
    b1, b2 = (fkx + 0.5) * 64.0, (fky + 0.5) * 64.0
    for t1 in range(8):
        one, two = speeds(cos_sin((fx + Z[t1]) * 0.125), turn2)
        back = root(one * (b1 * b1) + two * (b2 * b2))
        for s in range(8):
            linear = (2.0 * fx + 0.5) * Z[s] + (Z[t1] * (Z[s] - 0.5)) + half_x
            left[t1, s] = fraction(linear - back)
            first[t1, s] = one * squares1[s]
            second[t1, s] = two * squares2[s]

    def switch_row(step, _):
        t1, s1 = step // 8, step % 8
        turn1 = left[t1, s1]
        rad1 = first[t1, s1]
        for s2 in range(8):
            turns = turn1 + right[s1, s2] + root(rad1 + second[t1, s2])
            cosine, sine = cos_sin(turns, 1.0 / 64.0)
            k_cos[t1, s1 * 8 + s2] = cosine
            k_dif[t1, s1 * 8 + s2] = sine - cosine
            k_sum[t1, s1 * 8 + s2] = sine + cosine
        return 0

    lax.fori_loop(0, 64, switch_row, 0)

    space = from_scalars(space_ref, base, 32)
    wave = from_scalars(wave_ref, base, 32)
    ix, iy = space // 32, space % 32
    for bit_x, bit_y in ((z % 2, z // 2), (u1x, u1y), (u2x, u2y)):
        ix, iy = 2 * ix + bit_x, 2 * iy + bit_y
    fx, fy = ix.astype(F32), iy.astype(F32)
    fkx = (wave // 16 - 8).astype(F32) + 0.5
    fky = (wave % 16 - 8).astype(F32) + 0.5
    halves = ((ix + iy) & 1).astype(F32) * 0.5
    turn2 = cos_sin((fy + node) * 0.03125)
    b1, b2 = fkx * 256.0, fky * 256.0
    for t1 in range(8):
        one, two = speeds(cos_sin((fx + Z[t1]) * 0.03125), turn2)
        turns = halves + fkx * Z[t1] + fky * node + root(one * (b1 * b1) + two * (b2 * b2))
        cosine, sine = cos_sin(turns)
        rc[pl.ds(8 * t1, 8), :] = cosine
        rs[pl.ds(8 * t1, 8), :] = sine


def split(value):
    high = value.astype(BF16)
    return high, (value - high.astype(F32)).astype(BF16)


def dot(a, b):
    return jnp.dot(a, b, preferred_element_type=F32)


def main_kernel(y0, y1, y2, y3, ec, es, k_cos, k_dif, k_sum, merge_high, merge_low, out, turned_high, turned_low, merged, rows, sums):
    z = lax.axis_index("dev") % 4
    for u0 in range(4):
        for distance, y in enumerate((y0, y1, y2, y3)):
            child = (z + 4 - distance) % 4
            start = pl.multiple_of(child * 64, 64)
            for half in range(4):
                spot = pl.ds(16 * half, 16)
                cosine, sine = ec[u0, child, spot, :], es[u0, child, spot, :]
                for low in range(2):
                    re, im = y[0, low, spot, :], y[1, low, spot, :]
                    for part, value in enumerate((re * cosine - im * sine, re * sine + im * cosine)):
                        high, rest = split(value)
                        columns = pl.ds((2 * part + low) * 128, 128)
                        turned_high[pl.ds(start + 16 * half, 16), columns] = high
                        turned_low[pl.ds(start + 16 * half, 16), columns] = rest
        merged[u0] = (
            dot(merge_high[...], turned_high[...])
            + dot(merge_high[...], turned_low[...])
            + dot(merge_low[...], turned_high[...])
        )

    for low in range(2):
        for tile in range(8):
            spot = pl.ds(8 * tile, 8)
            re = swap_digit([merged[u0, spot, pl.ds(low * 128, 128)] for u0 in range(4)], 2, 8)
            im = swap_digit([merged[u0, spot, pl.ds((2 + low) * 128, 128)] for u0 in range(4)], 2, 8)
            for high in range(4):
                rows[0, 2 * high + low, spot, :] = re[high]
                rows[1, 2 * high + low, spot, :] = im[high]
                rows[2, 2 * high + low, spot, :] = re[high] + im[high]

    tiles, wide = 4, 2

    def block(step, _):
        t_base = step // (8 // wide) * tiles
        k_base = step % (8 // wide) * wide

        def chunk(index, total):
            total = list(total)
            for offset in range(8):
                s = index * 8 + offset
                values = []
                for k in range(wide):
                    values.append([jnp.broadcast_to(rows[i, k_base + k, pl.ds(s, 1), :], (8, 128)) for i in range(3)])
                for t in range(tiles):
                    cosine, dif, both = k_cos[t_base + t, s], k_dif[t_base + t, s], k_sum[t_base + t, s]
                    for k in range(wide):
                        at = 3 * (t * wide + k)
                        total[at] = total[at] + cosine * values[k][2]
                        total[at + 1] = total[at + 1] + dif * values[k][0]
                        total[at + 2] = total[at + 2] + both * values[k][1]
            return tuple(total)

        zero = jnp.zeros((8, 128), F32)
        total = lax.fori_loop(0, 8, chunk, (zero,) * (3 * tiles * wide))
        for t in range(tiles):
            for k in range(wide):
                at = 3 * (t * wide + k)
                sums[t_base + t, k_base + k] = total[at] - total[at + 2]
                sums[t_base + t, 8 + k_base + k] = total[at] + total[at + 1]
        return 0

    lax.fori_loop(0, (8 // tiles) * (8 // wide), block, 0)

    lane = lanes()
    upper = lane < 64
    even = lane // 32 % 2 == 0
    for tile in range(8):
        entry = [sums[tile, e] for e in range(16)]
        entry = [
            jnp.where(upper, entry[e], entry[e + 8]) + pltpu.roll(jnp.where(upper, entry[e + 8], entry[e]), 64, 1)
            for e in range(8)
        ]
        entry = [
            jnp.where(even, entry[e], entry[e + 4])
            + jnp.where(even, pltpu.roll(entry[e], 96, 1), pltpu.roll(entry[e + 4], 32, 1))
            for e in range(4)
        ]
        for u0, value in enumerate(swap_digit(entry, 2, 8)):
            out[u0, pl.ds(8 * tile, 8), :] = value


def sum_kernel(own, other, out0, out1, out2, out3):
    z = lax.axis_index("dev") % 4
    for distance, out in enumerate((out0, out1, out2, out3)):
        target = (z + distance) % 4
        out[...] = own[target] + other[target]


def last_kernel(r0, r1, r2, r3, spread_high, spread_low, rc, rs, out, high_ref, low_ref, spreaded):
    group = lax.axis_index("grp")
    z = lax.axis_index("dev") % 4
    for distance, r in enumerate((r0, r1, r2, r3)):
        source = (z + 4 - distance) % 4
        high, low = split(r[...])
        high_ref[source] = high
        low_ref[source] = low
    for source in range(4):
        spreaded[source] = (
            dot(spread_high[group], high_ref[source])
            + dot(spread_high[group], low_ref[source])
            + dot(spread_low[group], high_ref[source])
        )
    for tile in range(8):
        entry = [spreaded[q % 4, pl.ds(q // 4 * 64 + 8 * tile, 8), :] for q in range(16)]
        entry = swap_digit(entry, 4, 8)
        spot = pl.ds(8 * tile, 8)
        cosine, sine = rc[spot, :], rs[spot, :]
        for k in range(8):
            re, im = entry[k], entry[8 + k]
            out[0, k, spot, :] = re * cosine - im * sine
            out[1, k, spot, :] = re * sine + im * cosine


def call(kernel, inputs, outs, scratch=(), flops=0):
    return pl.pallas_call(
        kernel,
        out_shape=outs,
        in_specs=[spec for spec, _ in inputs],
        out_specs=jax.tree.map(lambda _: VMEM, outs),
        scratch_shapes=scratch,
        cost_estimate=pl.CostEstimate(flops=flops, bytes_accessed=1 << 20, transcendentals=0),
        compiler_params=pltpu.CompilerParams(vmem_limit_bytes=40 << 20),
    )(*[value for _, value in inputs])


def shape(*dims, kind=F32):
    return jax.ShapeDtypeStruct(dims, kind)


def along_z(value, distance):
    route = [(low, low // 4 * 4 + (low + distance) % 4) for low in range(lax.axis_size("dev"))]
    return lax.ppermute(value, "dev", route)


def across_groups(value, bit):
    return lax.ppermute(value, "grp", [(low, low ^ bit) for low in range(4)])


def per_device(coefficients, spatial_root, frequency_root):
    packed = call(
        pack_kernel,
        [(VMEM, coefficients)],
        [shape(2, 2, 64, 128)] * 4,
        [pltpu.VMEM((4, 2, 2, 64, 128), F32)],
        flops=1 << 20,
    )
    arrived = [packed[0]] + [along_z(packed[distance], distance) for distance in (1, 2, 3)]
    tables = call(
        table_kernel,
        [(SMEM, spatial_root), (SMEM, frequency_root)],
        [shape(4, 4, 64, 128)] * 2 + [shape(8, 64, 8, 128)] * 3 + [shape(64, 128)] * 2,
        [pltpu.VMEM((8, 8, 8, 128), F32)] * 4,
        flops=1 << 26,
    )
    ec, es, k_cos, k_dif, k_sum, rc, rs = tables
    merge_high, merge_low = in_two(MERGE)
    spread_high, spread_low = in_two(SPREAD)
    partial = call(
        main_kernel,
        [(VMEM, value) for value in (*arrived, ec, es, k_cos, k_dif, k_sum, merge_high, merge_low)],
        shape(4, 64, 128),
        [
            pltpu.VMEM((256, 512), BF16),
            pltpu.VMEM((256, 512), BF16),
            pltpu.VMEM((4, 64, 512), F32),
            pltpu.VMEM((3, 8, 64, 128), F32),
            pltpu.VMEM((8, 16, 8, 128), F32),
        ],
        flops=1 << 27,
    )
    partial = partial + across_groups(partial, 1)
    summed = call(
        sum_kernel,
        [(VMEM, partial), (VMEM, across_groups(partial, 2))],
        [shape(64, 128)] * 4,
        flops=1 << 18,
    )
    blocks = [summed[0]] + [along_z(summed[distance], distance) for distance in (1, 2, 3)]
    return call(
        last_kernel,
        [(VMEM, value) for value in (*blocks, spread_high, spread_low, rc, rs)],
        shape(2, 8, 64, 128),
        [pltpu.VMEM((4, 64, 128), BF16), pltpu.VMEM((4, 64, 128), BF16), pltpu.VMEM((4, 256, 128), F32)],
        flops=1 << 24,
    )


def solution(mesh):
    return jax.shard_map(
        per_device,
        mesh=mesh,
        in_specs=(P(None, None, None, ("grp", "dev")), P(), P()),
        out_specs=P(None, None, None, ("grp", "dev")),
        check_vma=False,
    )
```

```python
import functools

import jax
import jax.numpy as jnp
import numpy as np
from jax import lax
from jax.experimental import pallas as pl
from jax.experimental.pallas import tpu as pltpu
from jax.sharding import PartitionSpec as P


F32 = jnp.float32
BF16 = jnp.bfloat16
VMEM = pl.BlockSpec(memory_space=pltpu.VMEM)
HBM = pl.BlockSpec(memory_space=pltpu.HBM)

COS = (0.99999922, -19.73898252, 64.92872662, -85.27239701, 58.79403871, -21.07678212)
SIN = (6.28318282, -41.3414214, 81.59618388, -76.58010057, 41.20539503, -12.27126259)

NODES = 0.5 - 0.5 * np.cos(np.pi * (2.0 * np.arange(8) + 1.0) / 16.0)
Z = [float(node) for node in NODES]


def lagrange_table(half_cell):
    target = (NODES + half_cell) / 2.0
    table = np.ones((8, 8))
    for s in range(8):
        for n in range(8):
            if n != s:
                table[:, s] *= (target - NODES[n]) / (NODES[s] - NODES[n])
    return table


HALVES = [lagrange_table(0.0), lagrange_table(1.0)]
V = [np.kron(HALVES[u % 2], HALVES[u // 2]) for u in range(4)]
MERGE = np.concatenate([table.T for table in V], axis=1)
SPREAD = np.stack([np.concatenate([V[u2] @ V[u1] for u2 in range(4)]) for u1 in range(4)])


def in_two(table, axis=0):
    whole = table.astype(np.float32)
    high = whole.astype(BF16)
    low = (whole - high.astype(np.float32)).astype(BF16)
    return jnp.asarray(np.stack([high, low], axis=axis))


def polynomial(square, terms, scale):
    value = jnp.full_like(square, terms[-1] * scale)
    for term in terms[-2::-1]:
        value = value * square + term * scale
    return value


def fraction(turns):
    return turns - jnp.round(turns)


def cos_sin(turns, scale=1.0):
    part = fraction(turns)
    square = part * part
    return polynomial(square, COS, scale), part * polynomial(square, SIN, scale)


def root(value):
    return value * lax.rsqrt(value)


def speeds(first_cos_sin, second_cos_sin):
    one = (2.0 + first_cos_sin[1] * second_cos_sin[1]) * (1.0 / 16.0)
    two = (2.0 + first_cos_sin[0] * second_cos_sin[0]) * (1.0 / 16.0)
    return one * one, two * two


def lanes():
    return lax.broadcasted_iota(jnp.int32, (8, 128), 1)


def by_sublane(values):
    row = lax.broadcasted_iota(jnp.int32, (8, 128), 0)
    out = jnp.full((8, 128), values[0], F32)
    for index in range(1, 8):
        out = jnp.where(row == index, values[index], out)
    return out


def from_scalars(ref, base, period):
    place = lanes() % period
    out = jnp.full((8, 128), ref[base], jnp.int32)
    for index in range(1, period):
        out = jnp.where(place == index, ref[base + index], out)
    return out


def swap_four(parts, first_lane):
    digit = lax.broadcasted_iota(jnp.int32, parts[0].shape, parts[0].ndim - 1) // first_lane % 4
    out = []
    for target in range(4):
        value = parts[target]
        for index in range(4):
            if index != target:
                moved = pltpu.roll(parts[index], first_lane * (index - target) % 128, value.ndim - 1)
                value = jnp.where(digit == index, moved, value)
        out.append(value)
    return out


def swap_digit(parts, bits, first_lane):
    lane = lax.broadcasted_iota(jnp.int32, parts[0].shape, parts[0].ndim - 1)
    parts = list(parts)
    for bit in range(bits):
        step = 1 << bit
        shift = first_lane << bit
        low = lane // shift % 2 == 0
        for index in range(len(parts)):
            if index & step:
                continue
            a, b = parts[index], parts[index | step]
            axis = a.ndim - 1
            parts[index] = jnp.where(low, a, pltpu.roll(b, shift, axis))
            parts[index | step] = jnp.where(low, pltpu.roll(a, 128 - shift, axis), b)
    return parts


def pack_kernel(source, out0, out1, out2, out3, x_ref, held, sems):
    z = lax.axis_index("dev") % 4
    copies = [pltpu.make_async_copy(source.at[part], x_ref.at[part], sems.at[part]) for part in range(2)]
    for copy in copies:
        copy.start()
    for part in range(2):
        copies[part].wait()
        for low in range(2):
            for tile in range(8):
                rows = pl.ds(8 * tile, 8)
                group = [x_ref[part, 2 * high + low, rows, :] for high in range(4)]
                for target, value in enumerate(swap_four(group, 8)):
                    held[target, part, low, rows, :] = value
    for distance, out in enumerate((out0, out1, out2, out3)):
        target = (z + distance) % 4
        out[...] = held[target]


def table_kernel(
    space_hbm, wave_hbm, merge_hbm, spread_hbm,
    ec, es, switch, rc, rs, merge, spread,
    space_ref, wave_ref, first, second, left, right, sems,
):
    group = lax.axis_index("grp")
    device = lax.axis_index("dev")
    copies = [
        pltpu.make_async_copy(space_hbm, space_ref, sems.at[0]),
        pltpu.make_async_copy(wave_hbm, wave_ref, sems.at[1]),
        pltpu.make_async_copy(merge_hbm, merge, sems.at[2]),
        pltpu.make_async_copy(spread_hbm.at[group], spread, sems.at[3]),
    ]
    for copy in copies:
        copy.start()
    for copy in copies[:2]:
        copy.wait()
    z = device % 4
    base = device // 4 * 32
    lane = lanes()
    node = by_sublane(Z)
    u1x, u1y = group % 2, group // 2
    u2 = lane // 32
    u2x, u2y = u2 % 2, u2 // 2

    space = from_scalars(space_ref, base + z * 8, 8)
    wave = from_scalars(wave_ref, base + z * 8, 8)
    space_x, space_y = space // 32, space % 32
    wave_x, wave_y = wave // 16, wave % 16

    for u0 in range(4):
        ix, iy = 2 * space_x + u0 % 2, 2 * space_y + u0 // 2
        fx, fy = ix.astype(F32) + 0.5, iy.astype(F32) + 0.5
        one, two = speeds(cos_sin(fx * 0.125), cos_sin(fy * 0.125))
        for c in range(4):
            kx = wave_x * 8 + u2x * 4 + u1x * 2 + c % 2 - 64
            ky = wave_y * 8 + u2y * 4 + u1y * 2 + c // 2 - 64
            whole = (((2 * ix + 1) * kx + (2 * iy + 1) * ky) & 3).astype(F32) * 0.25
            fkx, fky = kx.astype(F32), ky.astype(F32)
            k2 = (fky + node) * 32.0
            part2 = whole + fy * 0.5 * node
            rad2 = two * (k2 * k2)
            for s1 in range(8):
                k1 = (fkx + Z[s1]) * 32.0
                turns = part2 + fx * (0.5 * Z[s1]) + root(one * (k1 * k1) + rad2)
                cosine, sine = cos_sin(turns)
                ec[u0, c, pl.ds(8 * s1, 8), :] = cosine
                es[u0, c, pl.ds(8 * s1, 8), :] = -sine

    u0 = lane // 8 % 4
    ix, iy = 2 * space_x + u0 % 2, 2 * space_y + u0 // 2
    kx, ky = wave_x * 4 + u2x * 2 + u1x - 32, wave_y * 4 + u2y * 2 + u1y - 32
    fx, fy = ix.astype(F32), iy.astype(F32)
    fkx, fky = kx.astype(F32), ky.astype(F32)
    half_x = ((kx + ix) & 1).astype(F32) * 0.5
    half_y = ((ky + iy) & 1).astype(F32) * 0.5
    one_a, two_a = speeds(cos_sin((fx + 0.5) * 0.125), cos_sin((fy + 0.5) * 0.125))
    turn2 = cos_sin((fy + node) * 0.125)
    squares1, squares2 = [], []
    for s in range(8):
        k1, k2 = (fkx + Z[s]) * 64.0, (fky + Z[s]) * 64.0
        squares1.append(k1 * k1)
        squares2.append(k2 * k2)
    for s1 in range(8):
        for s2 in range(8):
            linear = (2.0 * fy + 0.5) * Z[s2] + node * (Z[s2] - 0.5) + half_y
            right[s1, s2] = fraction(linear + root(one_a * squares1[s1] + two_a * squares2[s2]))
    b1, b2 = (fkx + 0.5) * 64.0, (fky + 0.5) * 64.0
    for t1 in range(8):
        one, two = speeds(cos_sin((fx + Z[t1]) * 0.125), turn2)
        back = root(one * (b1 * b1) + two * (b2 * b2))
        for s in range(8):
            linear = (2.0 * fx + 0.5) * Z[s] + (Z[t1] * (Z[s] - 0.5)) + half_x
            left[t1, s] = fraction(linear - back)
            first[t1, s] = one * squares1[s]
            second[t1, s] = two * squares2[s]

    def switch_row(step, _):
        t1, s1 = step // 8, step % 8
        turn1 = left[t1, s1]
        rad1 = first[t1, s1]
        for s2 in range(8):
            turns = turn1 + right[s1, s2] + root(rad1 + second[t1, s2])
            cosine, sine = cos_sin(turns, 1.0 / 64.0)
            switch[t1, s1 * 8 + s2, 0] = cosine
            switch[t1, s1 * 8 + s2, 1] = sine - cosine
            switch[t1, s1 * 8 + s2, 2] = sine + cosine
        return 0

    lax.fori_loop(0, 64, switch_row, 0)

    space = from_scalars(space_ref, base, 32)
    wave = from_scalars(wave_ref, base, 32)
    ix, iy = space // 32, space % 32
    for bit_x, bit_y in ((z % 2, z // 2), (u1x, u1y), (u2x, u2y)):
        ix, iy = 2 * ix + bit_x, 2 * iy + bit_y
    fx, fy = ix.astype(F32), iy.astype(F32)
    fkx = (wave // 16 - 8).astype(F32) + 0.5
    fky = (wave % 16 - 8).astype(F32) + 0.5
    halves = ((ix + iy) & 1).astype(F32) * 0.5
    turn2 = cos_sin((fy + node) * 0.03125)
    b1, b2 = fkx * 256.0, fky * 256.0
    for t1 in range(8):
        one, two = speeds(cos_sin((fx + Z[t1]) * 0.03125), turn2)
        turns = halves + fkx * Z[t1] + fky * node + root(one * (b1 * b1) + two * (b2 * b2))
        cosine, sine = cos_sin(turns)
        rc[pl.ds(8 * t1, 8), :] = cosine
        rs[pl.ds(8 * t1, 8), :] = sine
    for copy in copies[2:]:
        copy.wait()


def split(value):
    high = value.astype(BF16)
    return high, (value - high.astype(F32)).astype(BF16)


def dot(a, b):
    return jnp.dot(a, b, preferred_element_type=F32)


def main_kernel(y0, y1, y2, y3, ec, es, switch, merge, out, turned_high, turned_low, merged, rows, sums):
    z = lax.axis_index("dev") % 4
    for u0 in range(4):
        for distance, y in enumerate((y0, y1, y2, y3)):
            child = (z + 4 - distance) % 4
            start = pl.multiple_of(child * 64, 64)
            for half in range(4):
                spot = pl.ds(16 * half, 16)
                cosine, sine = ec[u0, child, spot, :], es[u0, child, spot, :]
                for low in range(2):
                    re, im = y[0, low, spot, :], y[1, low, spot, :]
                    for part, value in enumerate((re * cosine - im * sine, re * sine + im * cosine)):
                        high, rest = split(value)
                        columns = pl.ds((2 * part + low) * 128, 128)
                        turned_high[pl.ds(start + 16 * half, 16), columns] = high
                        turned_low[pl.ds(start + 16 * half, 16), columns] = rest
        merged[u0] = (
            dot(merge[0], turned_high[...]) + dot(merge[0], turned_low[...]) + dot(merge[1], turned_high[...])
        )

    for low in range(2):
        for tile in range(8):
            spot = pl.ds(8 * tile, 8)
            re = swap_four([merged[u0, spot, pl.ds(low * 128, 128)] for u0 in range(4)], 8)
            im = swap_four([merged[u0, spot, pl.ds((2 + low) * 128, 128)] for u0 in range(4)], 8)
            for high in range(4):
                rows[0, 2 * high + low, spot, :] = re[high]
                rows[1, 2 * high + low, spot, :] = im[high]
                rows[2, 2 * high + low, spot, :] = re[high] + im[high]

    tiles, wide = 4, 2

    def block(step, _):
        t_base = step // (8 // wide) * tiles
        k_base = step % (8 // wide) * wide

        def chunk(index, total):
            total = list(total)
            for offset in range(8):
                s = index * 8 + offset
                values = []
                for k in range(wide):
                    values.append([jnp.broadcast_to(rows[i, k_base + k, pl.ds(s, 1), :], (8, 128)) for i in range(3)])
                for t in range(tiles):
                    cosine, dif, both = (switch[t_base + t, s, i] for i in range(3))
                    for k in range(wide):
                        at = 3 * (t * wide + k)
                        total[at] = total[at] + cosine * values[k][2]
                        total[at + 1] = total[at + 1] + dif * values[k][0]
                        total[at + 2] = total[at + 2] + both * values[k][1]
            return tuple(total)

        zero = jnp.zeros((8, 128), F32)
        total = lax.fori_loop(0, 8, chunk, (zero,) * (3 * tiles * wide))
        for t in range(tiles):
            for k in range(wide):
                at = 3 * (t * wide + k)
                sums[t_base + t, k_base + k] = total[at] - total[at + 2]
                sums[t_base + t, 8 + k_base + k] = total[at] + total[at + 1]
        return 0

    lax.fori_loop(0, (8 // tiles) * (8 // wide), block, 0)

    lane = lanes()
    upper = lane < 64
    even = lane // 32 % 2 == 0
    for tile in range(8):
        entry = [sums[tile, e] for e in range(16)]
        entry = [
            jnp.where(upper, entry[e], entry[e + 8]) + pltpu.roll(jnp.where(upper, entry[e + 8], entry[e]), 64, 1)
            for e in range(8)
        ]
        entry = [
            jnp.where(even, entry[e], entry[e + 4])
            + jnp.where(even, pltpu.roll(entry[e], 96, 1), pltpu.roll(entry[e + 4], 32, 1))
            for e in range(4)
        ]
        for u0, value in enumerate(swap_four(entry, 8)):
            out[u0, pl.ds(8 * tile, 8), :] = value


def sum_kernel(own, other, out0, out1, out2, out3):
    z = lax.axis_index("dev") % 4
    for distance, out in enumerate((out0, out1, out2, out3)):
        target = (z + distance) % 4
        out[...] = own[target] + other[target]


def last_kernel(r0, r1, r2, r3, spread, rc, rs, target, high_ref, low_ref, spreaded, out, sems):
    z = lax.axis_index("dev") % 4
    for distance, r in enumerate((r0, r1, r2, r3)):
        source = (z + 4 - distance) % 4
        high, low = split(r[...])
        high_ref[source] = high
        low_ref[source] = low
    for source in range(4):
        spreaded[source] = (
            dot(spread[0], high_ref[source]) + dot(spread[0], low_ref[source]) + dot(spread[1], high_ref[source])
        )
    copies = []
    for tile in range(8):
        entry = [spreaded[q % 4, pl.ds(q // 4 * 64 + 8 * tile, 8), :] for q in range(16)]
        entry = swap_digit(entry, 4, 8)
        spot = pl.ds(8 * tile, 8)
        cosine, sine = rc[spot, :], rs[spot, :]
        for k in range(8):
            re, im = entry[k], entry[8 + k]
            out[0, k, spot, :] = re * cosine - im * sine
            out[1, k, spot, :] = re * sine + im * cosine
        if tile % 2:
            rows = pl.ds(8 * tile - 8, 16)
            copies.append(pltpu.make_async_copy(out.at[:, :, rows, :], target.at[:, :, rows, :], sems.at[tile // 2]))
            copies[-1].start()
    for copy in copies:
        copy.wait()


def call(kernel, inputs, outs, scratch=(), flops=0, place=VMEM):
    return pl.pallas_call(
        kernel,
        out_shape=outs,
        in_specs=[spec for spec, _ in inputs],
        out_specs=jax.tree.map(lambda _: place, outs),
        scratch_shapes=scratch,
        cost_estimate=pl.CostEstimate(flops=flops, bytes_accessed=1 << 20, transcendentals=0),
        compiler_params=pltpu.CompilerParams(vmem_limit_bytes=40 << 20),
    )(*[value for _, value in inputs])


def in_hbm(value):
    return pltpu.with_memory_space_constraint(value, pltpu.HBM)


def shape(*dims, kind=F32):
    return jax.ShapeDtypeStruct(dims, kind)


def along_z(value, distance):
    route = [(low, low // 4 * 4 + (low + distance) % 4) for low in range(lax.axis_size("dev"))]
    return lax.ppermute(value, "dev", route)


def across_groups(value, bit):
    return lax.ppermute(value, "grp", [(low, low ^ bit) for low in range(4)])


def per_device(coefficients, spatial_root, frequency_root):
    packed = call(
        pack_kernel,
        [(HBM, in_hbm(coefficients))],
        [shape(2, 2, 64, 128)] * 4,
        [pltpu.VMEM((2, 8, 64, 128), F32), pltpu.VMEM((4, 2, 2, 64, 128), F32), pltpu.SemaphoreType.DMA((2,))],
        flops=1 << 20,
    )
    arrived = [packed[0]] + [along_z(packed[distance], distance) for distance in (1, 2, 3)]
    tables = call(
        table_kernel,
        [(HBM, in_hbm(value)) for value in (spatial_root, frequency_root, in_two(MERGE), in_two(SPREAD, 1))],
        [shape(4, 4, 64, 128)] * 2
        + [shape(8, 64, 3, 8, 128)]
        + [shape(64, 128)] * 2
        + [shape(2, 64, 256, kind=BF16), shape(2, 256, 64, kind=BF16)],
        [pltpu.SMEM((256,), jnp.int32)] * 2
        + [pltpu.VMEM((8, 8, 8, 128), F32)] * 4
        + [pltpu.SemaphoreType.DMA((4,))],
        flops=1 << 26,
    )
    ec, es, switch, rc, rs, merge, spread = tables
    partial = call(
        main_kernel,
        [(VMEM, value) for value in (*arrived, ec, es, switch, merge)],
        shape(4, 64, 128),
        [
            pltpu.VMEM((256, 512), BF16),
            pltpu.VMEM((256, 512), BF16),
            pltpu.VMEM((4, 64, 512), F32),
            pltpu.VMEM((3, 8, 64, 128), F32),
            pltpu.VMEM((8, 16, 8, 128), F32),
        ],
        flops=1 << 27,
    )
    partial = partial + across_groups(partial, 1)
    summed = call(
        sum_kernel,
        [(VMEM, partial), (VMEM, across_groups(partial, 2))],
        [shape(64, 128)] * 4,
        flops=1 << 18,
    )
    blocks = [summed[0]] + [along_z(summed[distance], distance) for distance in (1, 2, 3)]
    return call(
        last_kernel,
        [(VMEM, value) for value in (*blocks, spread, rc, rs)],
        shape(2, 8, 64, 128),
        [
            pltpu.VMEM((4, 64, 128), BF16),
            pltpu.VMEM((4, 64, 128), BF16),
            pltpu.VMEM((4, 256, 128), F32),
            pltpu.VMEM((2, 8, 64, 128), F32),
            pltpu.SemaphoreType.DMA((4,)),
        ],
        flops=1 << 24,
        place=HBM,
    )


def solution(mesh):
    return jax.shard_map(
        per_device,
        mesh=mesh,
        in_specs=(P(None, None, None, ("grp", "dev")), P(), P()),
        out_specs=P(None, None, None, ("grp", "dev")),
        check_vma=False,
    )
```

```python
import functools

import jax
import jax.numpy as jnp
import numpy as np
from jax import lax
from jax.experimental import pallas as pl
from jax.experimental.pallas import tpu as pltpu
from jax.sharding import PartitionSpec as P


F32 = jnp.float32
PITCH = 72
BF16 = jnp.bfloat16
VMEM = pl.BlockSpec(memory_space=pltpu.VMEM)
HBM = pl.BlockSpec(memory_space=pltpu.HBM)

COS = (0.99999922, -19.73898252, 64.92872662, -85.27239701, 58.79403871, -21.07678212)
SIN = (6.28318282, -41.3414214, 81.59618388, -76.58010057, 41.20539503, -12.27126259)

NODES = 0.5 - 0.5 * np.cos(np.pi * (2.0 * np.arange(8) + 1.0) / 16.0)
Z = [float(node) for node in NODES]


def lagrange_table(half_cell):
    target = (NODES + half_cell) / 2.0
    table = np.ones((8, 8))
    for s in range(8):
        for n in range(8):
            if n != s:
                table[:, s] *= (target - NODES[n]) / (NODES[s] - NODES[n])
    return table


HALVES = [lagrange_table(0.0), lagrange_table(1.0)]
V = [np.kron(HALVES[u % 2], HALVES[u // 2]) for u in range(4)]
MERGE = np.concatenate([table.T for table in V], axis=1)
SPREAD = np.stack([np.concatenate([V[u2] @ V[u1] for u2 in range(4)]) for u1 in range(4)])


def in_two(table, axis=0):
    whole = table.astype(np.float32)
    high = whole.astype(BF16)
    low = (whole - high.astype(np.float32)).astype(BF16)
    return jnp.asarray(np.stack([high, low], axis=axis))


def polynomial(square, terms, scale):
    value = jnp.full_like(square, terms[-1] * scale)
    for term in terms[-2::-1]:
        value = value * square + term * scale
    return value


def fraction(turns):
    return turns - jnp.round(turns)


def cos_sin(turns, scale=1.0):
    part = fraction(turns)
    square = part * part
    return polynomial(square, COS, scale), part * polynomial(square, SIN, scale)


def root(value):
    return value * lax.rsqrt(value)


def speeds(first_cos_sin, second_cos_sin):
    one = (2.0 + first_cos_sin[1] * second_cos_sin[1]) * (1.0 / 16.0)
    two = (2.0 + first_cos_sin[0] * second_cos_sin[0]) * (1.0 / 16.0)
    return one * one, two * two


def lanes():
    return lax.broadcasted_iota(jnp.int32, (8, 128), 1)


def by_sublane(values):
    row = lax.broadcasted_iota(jnp.int32, (8, 128), 0)
    out = jnp.full((8, 128), values[0], F32)
    for index in range(1, 8):
        out = jnp.where(row == index, values[index], out)
    return out


def from_scalars(ref, base, period):
    place = lanes() % period
    out = jnp.full((8, 128), ref[base], jnp.int32)
    for index in range(1, period):
        out = jnp.where(place == index, ref[base + index], out)
    return out


def swap_four(parts, first_lane):
    digit = lax.broadcasted_iota(jnp.int32, parts[0].shape, parts[0].ndim - 1) // first_lane % 4
    out = []
    for target in range(4):
        value = parts[target]
        for index in range(4):
            if index != target:
                moved = pltpu.roll(parts[index], first_lane * (index - target) % 128, value.ndim - 1)
                value = jnp.where(digit == index, moved, value)
        out.append(value)
    return out


def swap_digit(parts, bits, first_lane):
    lane = lax.broadcasted_iota(jnp.int32, parts[0].shape, parts[0].ndim - 1)
    parts = list(parts)
    for bit in range(bits):
        step = 1 << bit
        shift = first_lane << bit
        low = lane // shift % 2 == 0
        for index in range(len(parts)):
            if index & step:
                continue
            a, b = parts[index], parts[index | step]
            axis = a.ndim - 1
            parts[index] = jnp.where(low, a, pltpu.roll(b, shift, axis))
            parts[index | step] = jnp.where(low, pltpu.roll(a, 128 - shift, axis), b)
    return parts


def pack_kernel(source, out0, out1, out2, out3, x_ref, held, sems):
    z = lax.axis_index("dev") % 4
    copies = []
    for part in range(2):
        for low in range(2):
            piece = pl.ds(4 * low, 4)
            copies.append(
                pltpu.make_async_copy(source.at[part, piece], x_ref.at[part, piece], sems.at[2 * part + low])
            )
            copies[-1].start()
    for part in range(2):
        for low in range(2):
            copies[2 * part + low].wait()
            for tile in range(8):
                rows = pl.ds(8 * tile, 8)
                group = [x_ref[part, 4 * low + high, rows, :] for high in range(4)]
                for target, value in enumerate(swap_four(group, 8)):
                    held[target, part, low, rows, :] = value
    for distance, out in enumerate((out0, out1, out2, out3)):
        target = (z + distance) % 4
        out[...] = held[target]


def table_kernel(
    space_hbm, wave_hbm, merge_hbm, spread_hbm,
    ec, es, switch, rc, rs, merge, spread,
    space_ref, wave_ref, first, second, left, right, sems,
):
    group = lax.axis_index("grp")
    device = lax.axis_index("dev")
    copies = [
        pltpu.make_async_copy(space_hbm, space_ref, sems.at[0]),
        pltpu.make_async_copy(wave_hbm, wave_ref, sems.at[1]),
        pltpu.make_async_copy(merge_hbm, merge, sems.at[2]),
        pltpu.make_async_copy(spread_hbm.at[group], spread, sems.at[3]),
    ]
    for copy in copies:
        copy.start()
    for copy in copies[:2]:
        copy.wait()
    z = device % 4
    base = device // 4 * 32
    lane = lanes()
    node = by_sublane(Z)
    u1x, u1y = group % 2, group // 2
    u2 = lane // 32
    u2x, u2y = u2 % 2, u2 // 2

    space = from_scalars(space_ref, base + z * 8, 8)
    wave = from_scalars(wave_ref, base + z * 8, 8)
    space_x, space_y = space // 32, space % 32
    wave_x, wave_y = wave // 16, wave % 16

    for u0 in range(4):
        ix, iy = 2 * space_x + u0 % 2, 2 * space_y + u0 // 2
        fx, fy = ix.astype(F32) + 0.5, iy.astype(F32) + 0.5
        one, two = speeds(cos_sin(fx * 0.125), cos_sin(fy * 0.125))
        for c in range(4):
            kx = wave_x * 8 + u2x * 4 + u1x * 2 + c % 2 - 64
            ky = wave_y * 8 + u2y * 4 + u1y * 2 + c // 2 - 64
            whole = (((2 * ix + 1) * kx + (2 * iy + 1) * ky) & 3).astype(F32) * 0.25
            fkx, fky = kx.astype(F32), ky.astype(F32)
            k2 = (fky + node) * 32.0
            part2 = whole + fy * 0.5 * node
            rad2 = two * (k2 * k2)
            for s1 in range(8):
                k1 = (fkx + Z[s1]) * 32.0
                turns = part2 + fx * (0.5 * Z[s1]) + root(one * (k1 * k1) + rad2)
                cosine, sine = cos_sin(turns)
                ec[u0, c, pl.ds(8 * s1, 8), :] = cosine
                es[u0, c, pl.ds(8 * s1, 8), :] = -sine

    u0 = lane // 8 % 4
    ix, iy = 2 * space_x + u0 % 2, 2 * space_y + u0 // 2
    kx, ky = wave_x * 4 + u2x * 2 + u1x - 32, wave_y * 4 + u2y * 2 + u1y - 32
    fx, fy = ix.astype(F32), iy.astype(F32)
    fkx, fky = kx.astype(F32), ky.astype(F32)
    half_x = ((kx + ix) & 1).astype(F32) * 0.5
    half_y = ((ky + iy) & 1).astype(F32) * 0.5
    one_a, two_a = speeds(cos_sin((fx + 0.5) * 0.125), cos_sin((fy + 0.5) * 0.125))
    turn2 = cos_sin((fy + node) * 0.125)
    squares1, squares2 = [], []
    for s in range(8):
        k1, k2 = (fkx + Z[s]) * 64.0, (fky + Z[s]) * 64.0
        squares1.append(k1 * k1)
        squares2.append(k2 * k2)
    for s1 in range(8):
        for s2 in range(8):
            linear = (2.0 * fy + 0.5) * Z[s2] + node * (Z[s2] - 0.5) + half_y
            right[s1, s2] = fraction(linear + root(one_a * squares1[s1] + two_a * squares2[s2]))
    b1, b2 = (fkx + 0.5) * 64.0, (fky + 0.5) * 64.0
    for t1 in range(8):
        one, two = speeds(cos_sin((fx + Z[t1]) * 0.125), turn2)
        back = root(one * (b1 * b1) + two * (b2 * b2))
        for s in range(8):
            linear = (2.0 * fx + 0.5) * Z[s] + (Z[t1] * (Z[s] - 0.5)) + half_x
            left[t1, s] = fraction(linear - back)
            first[t1, s] = one * squares1[s]
            second[t1, s] = two * squares2[s]

    def switch_rows(s1, _):
        for s2 in range(8):
            cosines, sines = [], []
            for t1 in range(8):
                turns = left[t1, s1] + right[s1, s2] + root(first[t1, s1] + second[t1, s2])
                cosine, sine = cos_sin(turns, 1.0 / 64.0)
                cosines.append(cosine)
                sines.append(sine)
            turned = jnp.concatenate(cosines + sines).T
            for tile in range(16):
                switch[pl.ds(tile * 8 * PITCH + s1 * 8 + s2, 8, stride=PITCH), :] = turned[8 * tile : 8 * tile + 8]
        return 0

    lax.fori_loop(0, 8, switch_rows, 0)

    space = from_scalars(space_ref, base, 32)
    wave = from_scalars(wave_ref, base, 32)
    ix, iy = space // 32, space % 32
    for bit_x, bit_y in ((z % 2, z // 2), (u1x, u1y), (u2x, u2y)):
        ix, iy = 2 * ix + bit_x, 2 * iy + bit_y
    fx, fy = ix.astype(F32), iy.astype(F32)
    fkx = (wave // 16 - 8).astype(F32) + 0.5
    fky = (wave % 16 - 8).astype(F32) + 0.5
    halves = ((ix + iy) & 1).astype(F32) * 0.5
    turn2 = cos_sin((fy + node) * 0.03125)
    b1, b2 = fkx * 256.0, fky * 256.0
    for t1 in range(8):
        one, two = speeds(cos_sin((fx + Z[t1]) * 0.03125), turn2)
        turns = halves + fkx * Z[t1] + fky * node + root(one * (b1 * b1) + two * (b2 * b2))
        cosine, sine = cos_sin(turns)
        rc[pl.ds(8 * t1, 8), :] = cosine
        rs[pl.ds(8 * t1, 8), :] = sine
    for copy in copies[2:]:
        copy.wait()


def split(value):
    high = value.astype(BF16)
    return high, (value - high.astype(F32)).astype(BF16)


def dot(a, b):
    return jnp.dot(a, b, preferred_element_type=F32)


def main_kernel(y0, y1, y2, y3, ec, es, switch, merge, out, turned_high, turned_low, merged, rows, turned, sums):
    z = lax.axis_index("dev") % 4
    for u0 in range(4):
        for distance, y in enumerate((y0, y1, y2, y3)):
            child = (z + 4 - distance) % 4
            start = pl.multiple_of(child * 64, 64)
            for half in range(4):
                spot = pl.ds(16 * half, 16)
                cosine, sine = ec[u0, child, spot, :], es[u0, child, spot, :]
                for low in range(2):
                    re, im = y[0, low, spot, :], y[1, low, spot, :]
                    for part, value in enumerate((re * cosine - im * sine, re * sine + im * cosine)):
                        high, rest = split(value)
                        columns = pl.ds((2 * part + low) * 128, 128)
                        turned_high[pl.ds(start + 16 * half, 16), columns] = high
                        turned_low[pl.ds(start + 16 * half, 16), columns] = rest
        merged[u0] = (
            dot(merge[0], turned_high[...]) + dot(merge[0], turned_low[...]) + dot(merge[1], turned_high[...])
        )

    for low in range(2):
        for tile in range(8):
            spot = pl.ds(8 * tile, 8)
            re = swap_four([merged[u0, spot, pl.ds(low * 128, 128)] for u0 in range(4)], 8)
            im = swap_four([merged[u0, spot, pl.ds((2 + low) * 128, 128)] for u0 in range(4)], 8)
            for high in range(4):
                rows[4 * low + high, spot, :] = re[high]
                rows[4 * low + high, pl.ds(64 + 8 * tile, 8), :] = im[high]

    for k in range(8):
        flat = rows[k].T
        for tile in range(16):
            turned[pl.ds(tile * 64 + k, 8, stride=8), :] = flat[8 * tile : 8 * tile + 8]

    lane = lanes()
    left = lane < 64
    for u0 in range(4):
        for r in range(8):
            pair = [u2 * 32 + u0 * 8 + r for u2 in range(4)]
            value = [turned[pl.ds(8 * m, 8), :] for m in pair]
            other = [pltpu.roll(v, 64, 1) for v in value]
            re = [jnp.where(left, value[u], other[u + 1]) for u in (0, 2)]
            im = [jnp.where(left, other[u], value[u + 1]) for u in (0, 2)]
            high, low = split(jnp.concatenate([jnp.concatenate(re, axis=1), jnp.concatenate(im, axis=1)]))
            matrix_high, matrix_low = split(jnp.concatenate([switch[pl.ds(PITCH * m, 64), :] for m in pair]))
            product = dot(high, matrix_high) + dot(low, matrix_high) + dot(high, matrix_low)
            crossed = pltpu.roll(product[8:], 64, 1)
            total = product[:8] + jnp.where(left, -crossed, crossed)
            sums[u0, pl.ds(r, 8, stride=8), :] = total
            sums[u0, pl.ds(64 + r, 8, stride=8), :] = pltpu.roll(total, 64, 1)
    for u0 in range(4):
        out[u0] = sums[u0].T[:64]


def sum_kernel(own, other, out0, out1, out2, out3):
    z = lax.axis_index("dev") % 4
    for distance, out in enumerate((out0, out1, out2, out3)):
        target = (z + distance) % 4
        out[...] = own[target] + other[target]


def last_kernel(r0, r1, r2, r3, spread, rc, rs, target, high_ref, low_ref, spreaded, out, sems):
    z = lax.axis_index("dev") % 4
    for distance, r in enumerate((r0, r1, r2, r3)):
        source = (z + 4 - distance) % 4
        high, low = split(r[...])
        high_ref[source] = high
        low_ref[source] = low
    for source in range(4):
        spreaded[source] = (
            dot(spread[0], high_ref[source]) + dot(spread[0], low_ref[source]) + dot(spread[1], high_ref[source])
        )
    copies = []
    for tile in range(8):
        entry = [spreaded[q % 4, pl.ds(q // 4 * 64 + 8 * tile, 8), :] for q in range(16)]
        entry = swap_digit(entry, 4, 8)
        spot = pl.ds(8 * tile, 8)
        cosine, sine = rc[spot, :], rs[spot, :]
        for k in range(8):
            re, im = entry[k], entry[8 + k]
            out[0, k, spot, :] = re * cosine - im * sine
            out[1, k, spot, :] = re * sine + im * cosine
        if tile % 2:
            rows = pl.ds(8 * tile - 8, 16)
            copies.append(pltpu.make_async_copy(out.at[:, :, rows, :], target.at[:, :, rows, :], sems.at[tile // 2]))
            copies[-1].start()
    for copy in copies:
        copy.wait()


def call(kernel, inputs, outs, scratch=(), flops=0, place=VMEM):
    return pl.pallas_call(
        kernel,
        out_shape=outs,
        in_specs=[spec for spec, _ in inputs],
        out_specs=jax.tree.map(lambda _: place, outs),
        scratch_shapes=scratch,
        cost_estimate=pl.CostEstimate(flops=flops, bytes_accessed=1 << 20, transcendentals=0),
        compiler_params=pltpu.CompilerParams(vmem_limit_bytes=40 << 20),
    )(*[value for _, value in inputs])


def in_hbm(value):
    return pltpu.with_memory_space_constraint(value, pltpu.HBM)


def shape(*dims, kind=F32):
    return jax.ShapeDtypeStruct(dims, kind)


def along_z(value, distance):
    route = [(low, low // 4 * 4 + (low + distance) % 4) for low in range(lax.axis_size("dev"))]
    return lax.ppermute(value, "dev", route)


def across_groups(value, bit):
    return lax.ppermute(value, "grp", [(low, low ^ bit) for low in range(4)])


def per_device(coefficients, spatial_root, frequency_root):
    packed = call(
        pack_kernel,
        [(HBM, in_hbm(coefficients))],
        [shape(2, 2, 64, 128)] * 4,
        [pltpu.VMEM((2, 8, 64, 128), F32), pltpu.VMEM((4, 2, 2, 64, 128), F32), pltpu.SemaphoreType.DMA((4,))],
        flops=1 << 20,
    )
    arrived = [packed[0]] + [along_z(packed[distance], distance) for distance in (1, 2, 3)]
    tables = call(
        table_kernel,
        [(HBM, in_hbm(value)) for value in (spatial_root, frequency_root, in_two(MERGE), in_two(SPREAD, 1))],
        [shape(4, 4, 64, 128)] * 2
        + [shape(128 * PITCH, 128)]
        + [shape(64, 128)] * 2
        + [shape(2, 64, 256, kind=BF16), shape(2, 256, 64, kind=BF16)],
        [pltpu.SMEM((256,), jnp.int32)] * 2
        + [pltpu.VMEM((8, 8, 8, 128), F32)] * 4
        + [pltpu.SemaphoreType.DMA((4,))],
        flops=1 << 26,
    )
    ec, es, switch, rc, rs, merge, spread = tables
    partial = call(
        main_kernel,
        [(VMEM, value) for value in (*arrived, ec, es, switch, merge)],
        shape(4, 64, 128),
        [
            pltpu.VMEM((256, 512), BF16),
            pltpu.VMEM((256, 512), BF16),
            pltpu.VMEM((4, 64, 512), F32),
            pltpu.VMEM((8, 128, 128), F32),
            pltpu.VMEM((1024, 128), F32),
            pltpu.VMEM((4, 128, 128), F32),
        ],
        flops=1 << 27,
    )
    partial = partial + across_groups(partial, 1)
    summed = call(
        sum_kernel,
        [(VMEM, partial), (VMEM, across_groups(partial, 2))],
        [shape(64, 128)] * 4,
        flops=1 << 18,
    )
    blocks = [summed[0]] + [along_z(summed[distance], distance) for distance in (1, 2, 3)]
    return call(
        last_kernel,
        [(VMEM, value) for value in (*blocks, spread, rc, rs)],
        shape(2, 8, 64, 128),
        [
            pltpu.VMEM((4, 64, 128), BF16),
            pltpu.VMEM((4, 64, 128), BF16),
            pltpu.VMEM((4, 256, 128), F32),
            pltpu.VMEM((2, 8, 64, 128), F32),
            pltpu.SemaphoreType.DMA((4,)),
        ],
        flops=1 << 24,
        place=HBM,
    )


def solution(mesh):
    return jax.shard_map(
        per_device,
        mesh=mesh,
        in_specs=(P(None, None, None, ("grp", "dev")), P(), P()),
        out_specs=P(None, None, None, ("grp", "dev")),
        check_vma=False,
    )
```

```python
import functools

import jax
import jax.numpy as jnp
import numpy as np
from jax import lax
from jax.experimental import pallas as pl
from jax.experimental.pallas import tpu as pltpu
from jax.sharding import PartitionSpec as P


F32 = jnp.float32
PITCH = 72
ORDER = (2, 1, 3, 0)
BF16 = jnp.bfloat16
VMEM = pl.BlockSpec(memory_space=pltpu.VMEM)
HBM = pl.BlockSpec(memory_space=pltpu.HBM)

COS = (0.99999922, -19.73898252, 64.92872662, -85.27239701, 58.79403871, -21.07678212)
SIN = (6.28318282, -41.3414214, 81.59618388, -76.58010057, 41.20539503, -12.27126259)

NODES = 0.5 - 0.5 * np.cos(np.pi * (2.0 * np.arange(8) + 1.0) / 16.0)
Z = [float(node) for node in NODES]


def lagrange_table(half_cell):
    target = (NODES + half_cell) / 2.0
    table = np.ones((8, 8))
    for s in range(8):
        for n in range(8):
            if n != s:
                table[:, s] *= (target - NODES[n]) / (NODES[s] - NODES[n])
    return table


HALVES = [lagrange_table(0.0), lagrange_table(1.0)]
V = [np.kron(HALVES[u % 2], HALVES[u // 2]) for u in range(4)]
MERGE = np.concatenate([table.T for table in V], axis=1)
SPREAD = np.stack([np.concatenate([V[u2] @ V[u1] for u2 in range(4)]) for u1 in range(4)])


def in_two(table, axis=0):
    whole = table.astype(np.float32)
    high = whole.astype(BF16)
    low = (whole - high.astype(np.float32)).astype(BF16)
    return jnp.asarray(np.stack([high, low], axis=axis))


def polynomial(square, terms, scale):
    value = jnp.full_like(square, terms[-1] * scale)
    for term in terms[-2::-1]:
        value = value * square + term * scale
    return value


def fraction(turns):
    return turns - jnp.round(turns)


def cos_sin(turns, scale=1.0):
    part = fraction(turns)
    square = part * part
    return polynomial(square, COS, scale), part * polynomial(square, SIN, scale)


def root(value):
    return value * lax.rsqrt(value)


def speeds(first_cos_sin, second_cos_sin):
    one = (2.0 + first_cos_sin[1] * second_cos_sin[1]) * (1.0 / 16.0)
    two = (2.0 + first_cos_sin[0] * second_cos_sin[0]) * (1.0 / 16.0)
    return one * one, two * two


def lanes():
    return lax.broadcasted_iota(jnp.int32, (8, 128), 1)


def by_sublane(values):
    row = lax.broadcasted_iota(jnp.int32, (8, 128), 0)
    out = jnp.full((8, 128), values[0], F32)
    for index in range(1, 8):
        out = jnp.where(row == index, values[index], out)
    return out


def from_scalars(ref, base, period):
    place = lanes() % period
    out = jnp.full((8, 128), ref[base], jnp.int32)
    for index in range(1, period):
        out = jnp.where(place == index, ref[base + index], out)
    return out


def swap_four(parts, first_lane):
    digit = lax.broadcasted_iota(jnp.int32, parts[0].shape, parts[0].ndim - 1) // first_lane % 4
    out = []
    for target in range(4):
        value = parts[target]
        for index in range(4):
            if index != target:
                moved = pltpu.roll(parts[index], first_lane * (index - target) % 128, value.ndim - 1)
                value = jnp.where(digit == index, moved, value)
        out.append(value)
    return out


def swap_digit(parts, bits, first_lane):
    lane = lax.broadcasted_iota(jnp.int32, parts[0].shape, parts[0].ndim - 1)
    parts = list(parts)
    for bit in range(bits):
        step = 1 << bit
        shift = first_lane << bit
        low = lane // shift % 2 == 0
        for index in range(len(parts)):
            if index & step:
                continue
            a, b = parts[index], parts[index | step]
            axis = a.ndim - 1
            parts[index] = jnp.where(low, a, pltpu.roll(b, shift, axis))
            parts[index | step] = jnp.where(low, pltpu.roll(a, 128 - shift, axis), b)
    return parts


def pack_kernel(source, out0, out1, out2, out3, x_ref, held, sems):
    z = lax.axis_index("dev") % 4
    copies = []
    for part in range(2):
        for low in range(2):
            piece = pl.ds(4 * low, 4)
            copies.append(
                pltpu.make_async_copy(source.at[part, piece], x_ref.at[part, piece], sems.at[2 * part + low])
            )
            copies[-1].start()
    for part in range(2):
        for low in range(2):
            copies[2 * part + low].wait()
            for tile in range(8):
                rows = pl.ds(8 * tile, 8)
                group = [x_ref[part, 4 * low + high, rows, :] for high in range(4)]
                for target, value in enumerate(swap_four(group, 8)):
                    held[target, part, low, rows, :] = value
    for distance, out in zip(ORDER, (out0, out1, out2, out3)):
        target = (z + distance) % 4
        out[...] = held[target]


def table_kernel(
    space_hbm, wave_hbm, merge_hbm, spread_hbm,
    ec, es, switch, rc, rs, merge, spread,
    space_ref, wave_ref, first, second, left, right, sems,
):
    group = lax.axis_index("grp")
    device = lax.axis_index("dev")
    copies = [
        pltpu.make_async_copy(space_hbm, space_ref, sems.at[0]),
        pltpu.make_async_copy(wave_hbm, wave_ref, sems.at[1]),
        pltpu.make_async_copy(merge_hbm, merge, sems.at[2]),
        pltpu.make_async_copy(spread_hbm.at[group], spread, sems.at[3]),
    ]
    for copy in copies:
        copy.start()
    for copy in copies[:2]:
        copy.wait()
    z = device % 4
    base = device // 4 * 32
    lane = lanes()
    node = by_sublane(Z)
    u1x, u1y = group % 2, group // 2
    u2 = lane // 32
    u2x, u2y = u2 % 2, u2 // 2

    space = from_scalars(space_ref, base + z * 8, 8)
    wave = from_scalars(wave_ref, base + z * 8, 8)
    space_x, space_y = space // 32, space % 32
    wave_x, wave_y = wave // 16, wave % 16

    for u0 in range(4):
        ix, iy = 2 * space_x + u0 % 2, 2 * space_y + u0 // 2
        fx, fy = ix.astype(F32) + 0.5, iy.astype(F32) + 0.5
        one, two = speeds(cos_sin(fx * 0.125), cos_sin(fy * 0.125))
        for c in range(4):
            kx = wave_x * 8 + u2x * 4 + u1x * 2 + c % 2 - 64
            ky = wave_y * 8 + u2y * 4 + u1y * 2 + c // 2 - 64
            whole = (((2 * ix + 1) * kx + (2 * iy + 1) * ky) & 3).astype(F32) * 0.25
            fkx, fky = kx.astype(F32), ky.astype(F32)
            k2 = (fky + node) * 32.0
            part2 = whole + fy * 0.5 * node
            rad2 = two * (k2 * k2)
            for s1 in range(8):
                k1 = (fkx + Z[s1]) * 32.0
                turns = part2 + fx * (0.5 * Z[s1]) + root(one * (k1 * k1) + rad2)
                cosine, sine = cos_sin(turns)
                ec[u0, c, pl.ds(8 * s1, 8), :] = cosine
                es[u0, c, pl.ds(8 * s1, 8), :] = -sine

    u0 = lane // 8 % 4
    ix, iy = 2 * space_x + u0 % 2, 2 * space_y + u0 // 2
    kx, ky = wave_x * 4 + u2x * 2 + u1x - 32, wave_y * 4 + u2y * 2 + u1y - 32
    fx, fy = ix.astype(F32), iy.astype(F32)
    fkx, fky = kx.astype(F32), ky.astype(F32)
    half_x = ((kx + ix) & 1).astype(F32) * 0.5
    half_y = ((ky + iy) & 1).astype(F32) * 0.5
    one_a, two_a = speeds(cos_sin((fx + 0.5) * 0.125), cos_sin((fy + 0.5) * 0.125))
    turn2 = cos_sin((fy + node) * 0.125)
    squares1, squares2 = [], []
    for s in range(8):
        k1, k2 = (fkx + Z[s]) * 64.0, (fky + Z[s]) * 64.0
        squares1.append(k1 * k1)
        squares2.append(k2 * k2)
    for s1 in range(8):
        for s2 in range(8):
            linear = (2.0 * fy + 0.5) * Z[s2] + node * (Z[s2] - 0.5) + half_y
            right[s1, s2] = fraction(linear + root(one_a * squares1[s1] + two_a * squares2[s2]))
    b1, b2 = (fkx + 0.5) * 64.0, (fky + 0.5) * 64.0
    for t1 in range(8):
        one, two = speeds(cos_sin((fx + Z[t1]) * 0.125), turn2)
        back = root(one * (b1 * b1) + two * (b2 * b2))
        for s in range(8):
            linear = (2.0 * fx + 0.5) * Z[s] + (Z[t1] * (Z[s] - 0.5)) + half_x
            left[t1, s] = fraction(linear - back)
            first[t1, s] = one * squares1[s]
            second[t1, s] = two * squares2[s]

    def switch_rows(s1, _):
        for s2 in range(8):
            cosines, sines = [], []
            for t1 in range(8):
                turns = left[t1, s1] + right[s1, s2] + root(first[t1, s1] + second[t1, s2])
                cosine, sine = cos_sin(turns, 1.0 / 64.0)
                cosines.append(cosine)
                sines.append(sine)
            turned = jnp.concatenate(cosines + sines).T
            for tile in range(16):
                switch[pl.ds(tile * 8 * PITCH + s1 * 8 + s2, 8, stride=PITCH), :] = turned[8 * tile : 8 * tile + 8]
        return 0

    lax.fori_loop(0, 8, switch_rows, 0)

    space = from_scalars(space_ref, base, 32)
    wave = from_scalars(wave_ref, base, 32)
    ix, iy = space // 32, space % 32
    for bit_x, bit_y in ((z % 2, z // 2), (u1x, u1y), (u2x, u2y)):
        ix, iy = 2 * ix + bit_x, 2 * iy + bit_y
    fx, fy = ix.astype(F32), iy.astype(F32)
    fkx = (wave // 16 - 8).astype(F32) + 0.5
    fky = (wave % 16 - 8).astype(F32) + 0.5
    halves = ((ix + iy) & 1).astype(F32) * 0.5
    turn2 = cos_sin((fy + node) * 0.03125)
    b1, b2 = fkx * 256.0, fky * 256.0
    for t1 in range(8):
        one, two = speeds(cos_sin((fx + Z[t1]) * 0.03125), turn2)
        turns = halves + fkx * Z[t1] + fky * node + root(one * (b1 * b1) + two * (b2 * b2))
        cosine, sine = cos_sin(turns)
        rc[pl.ds(8 * t1, 8), :] = cosine
        rs[pl.ds(8 * t1, 8), :] = sine
    for copy in copies[2:]:
        copy.wait()


def split(value):
    high = value.astype(BF16)
    return high, (value - high.astype(F32)).astype(BF16)


def dot(a, b):
    return jnp.dot(a, b, preferred_element_type=F32)


def main_kernel(y0, y1, y2, y3, ec, es, switch, merge, out, turned_high, turned_low, merged, rows, turned, sums):
    z = lax.axis_index("dev") % 4
    for u0 in range(4):
        for distance, y in zip(ORDER, (y0, y1, y2, y3)):
            child = (z + 4 - distance) % 4
            start = pl.multiple_of(child * 64, 64)
            for half in range(4):
                spot = pl.ds(16 * half, 16)
                cosine, sine = ec[u0, child, spot, :], es[u0, child, spot, :]
                for low in range(2):
                    re, im = y[0, low, spot, :], y[1, low, spot, :]
                    for part, value in enumerate((re * cosine - im * sine, re * sine + im * cosine)):
                        high, rest = split(value)
                        columns = pl.ds((2 * part + low) * 128, 128)
                        turned_high[pl.ds(start + 16 * half, 16), columns] = high
                        turned_low[pl.ds(start + 16 * half, 16), columns] = rest
        merged[u0] = (
            dot(merge[0], turned_high[...]) + dot(merge[0], turned_low[...]) + dot(merge[1], turned_high[...])
        )

    for low in range(2):
        for tile in range(8):
            spot = pl.ds(8 * tile, 8)
            re = swap_four([merged[u0, spot, pl.ds(low * 128, 128)] for u0 in range(4)], 8)
            im = swap_four([merged[u0, spot, pl.ds((2 + low) * 128, 128)] for u0 in range(4)], 8)
            for high in range(4):
                rows[4 * low + high, spot, :] = re[high]
                rows[4 * low + high, pl.ds(64 + 8 * tile, 8), :] = im[high]

    for k in range(8):
        flat = rows[k].T
        for tile in range(16):
            turned[pl.ds(tile * 64 + k, 8, stride=8), :] = flat[8 * tile : 8 * tile + 8]

    lane = lanes()
    left = lane < 64
    for u0 in range(4):
        for r in range(8):
            pair = [u2 * 32 + u0 * 8 + r for u2 in range(4)]
            value = [turned[pl.ds(8 * m, 8), :] for m in pair]
            other = [pltpu.roll(v, 64, 1) for v in value]
            re = [jnp.where(left, value[u], other[u + 1]) for u in (0, 2)]
            im = [jnp.where(left, other[u], value[u + 1]) for u in (0, 2)]
            high, low = split(jnp.concatenate([jnp.concatenate(re, axis=1), jnp.concatenate(im, axis=1)]))
            matrix_high, matrix_low = split(jnp.concatenate([switch[pl.ds(PITCH * m, 64), :] for m in pair]))
            product = dot(high, matrix_high) + dot(low, matrix_high) + dot(high, matrix_low)
            crossed = pltpu.roll(product[8:], 64, 1)
            total = product[:8] + jnp.where(left, -crossed, crossed)
            sums[u0, pl.ds(r, 8, stride=8), :] = total
            sums[u0, pl.ds(64 + r, 8, stride=8), :] = pltpu.roll(total, 64, 1)
    for u0 in range(4):
        out[u0] = sums[u0].T[:64]


def sum_kernel(own, other, out0, out1, out2, out3):
    z = lax.axis_index("dev") % 4
    for distance, out in zip(ORDER, (out0, out1, out2, out3)):
        target = (z + distance) % 4
        out[...] = own[target] + other[target]


def last_kernel(r0, r1, r2, r3, spread, rc, rs, target, high_ref, low_ref, spreaded, out, sems):
    z = lax.axis_index("dev") % 4
    for distance, r in zip(ORDER, (r0, r1, r2, r3)):
        source = (z + 4 - distance) % 4
        high, low = split(r[...])
        high_ref[source] = high
        low_ref[source] = low
    for source in range(4):
        spreaded[source] = (
            dot(spread[0], high_ref[source]) + dot(spread[0], low_ref[source]) + dot(spread[1], high_ref[source])
        )
    copies = []
    for tile in range(8):
        entry = [spreaded[q % 4, pl.ds(q // 4 * 64 + 8 * tile, 8), :] for q in range(16)]
        entry = swap_digit(entry, 4, 8)
        spot = pl.ds(8 * tile, 8)
        cosine, sine = rc[spot, :], rs[spot, :]
        for k in range(8):
            re, im = entry[k], entry[8 + k]
            out[0, k, spot, :] = re * cosine - im * sine
            out[1, k, spot, :] = re * sine + im * cosine
        if tile % 2:
            rows = pl.ds(8 * tile - 8, 16)
            copies.append(pltpu.make_async_copy(out.at[:, :, rows, :], target.at[:, :, rows, :], sems.at[tile // 2]))
            copies[-1].start()
    for copy in copies:
        copy.wait()


def call(kernel, inputs, outs, scratch=(), flops=0, place=VMEM):
    return pl.pallas_call(
        kernel,
        out_shape=outs,
        in_specs=[spec for spec, _ in inputs],
        out_specs=jax.tree.map(lambda _: place, outs),
        scratch_shapes=scratch,
        cost_estimate=pl.CostEstimate(flops=flops, bytes_accessed=1 << 20, transcendentals=0),
        compiler_params=pltpu.CompilerParams(vmem_limit_bytes=40 << 20),
    )(*[value for _, value in inputs])


def in_hbm(value):
    return pltpu.with_memory_space_constraint(value, pltpu.HBM)


def shape(*dims, kind=F32):
    return jax.ShapeDtypeStruct(dims, kind)


def along_z(value, distance):
    route = [(low, low // 4 * 4 + (low + distance) % 4) for low in range(lax.axis_size("dev"))]
    return lax.ppermute(value, "dev", route)


def exchange(pieces):
    return [along_z(piece, distance) if distance else piece for distance, piece in zip(ORDER, pieces)]


def across_groups(value, bit):
    return lax.ppermute(value, "grp", [(low, low ^ bit) for low in range(4)])


def per_device(coefficients, spatial_root, frequency_root):
    packed = call(
        pack_kernel,
        [(HBM, in_hbm(coefficients))],
        [shape(2, 2, 64, 128)] * 4,
        [pltpu.VMEM((2, 8, 64, 128), F32), pltpu.VMEM((4, 2, 2, 64, 128), F32), pltpu.SemaphoreType.DMA((4,))],
        flops=1 << 20,
    )
    arrived = exchange(packed)
    tables = call(
        table_kernel,
        [(HBM, in_hbm(value)) for value in (spatial_root, frequency_root, in_two(MERGE), in_two(SPREAD, 1))],
        [shape(4, 4, 64, 128)] * 2
        + [shape(128 * PITCH, 128)]
        + [shape(64, 128)] * 2
        + [shape(2, 64, 256, kind=BF16), shape(2, 256, 64, kind=BF16)],
        [pltpu.SMEM((256,), jnp.int32)] * 2
        + [pltpu.VMEM((8, 8, 8, 128), F32)] * 4
        + [pltpu.SemaphoreType.DMA((4,))],
        flops=1 << 26,
    )
    ec, es, switch, rc, rs, merge, spread = tables
    partial = call(
        main_kernel,
        [(VMEM, value) for value in (*arrived, ec, es, switch, merge)],
        shape(4, 64, 128),
        [
            pltpu.VMEM((256, 512), BF16),
            pltpu.VMEM((256, 512), BF16),
            pltpu.VMEM((4, 64, 512), F32),
            pltpu.VMEM((8, 128, 128), F32),
            pltpu.VMEM((1024, 128), F32),
            pltpu.VMEM((4, 128, 128), F32),
        ],
        flops=1 << 27,
    )
    partial = partial + across_groups(partial, 1)
    summed = call(
        sum_kernel,
        [(VMEM, partial), (VMEM, across_groups(partial, 2))],
        [shape(64, 128)] * 4,
        flops=1 << 18,
    )
    blocks = exchange(summed)
    return call(
        last_kernel,
        [(VMEM, value) for value in (*blocks, spread, rc, rs)],
        shape(2, 8, 64, 128),
        [
            pltpu.VMEM((4, 64, 128), BF16),
            pltpu.VMEM((4, 64, 128), BF16),
            pltpu.VMEM((4, 256, 128), F32),
            pltpu.VMEM((2, 8, 64, 128), F32),
            pltpu.SemaphoreType.DMA((4,)),
        ],
        flops=1 << 24,
        place=HBM,
    )


def solution(mesh):
    return jax.shard_map(
        per_device,
        mesh=mesh,
        in_specs=(P(None, None, None, ("grp", "dev")), P(), P()),
        out_specs=P(None, None, None, ("grp", "dev")),
        check_vma=False,
    )
```

```python
import functools

import jax
import jax.numpy as jnp
import numpy as np
from jax import lax
from jax.experimental import pallas as pl
from jax.experimental.pallas import tpu as pltpu
from jax.sharding import PartitionSpec as P


F32 = jnp.float32
PITCH = 72
ORDER = (2, 1, 3, 0)
BF16 = jnp.bfloat16
VMEM = pl.BlockSpec(memory_space=pltpu.VMEM)
HBM = pl.BlockSpec(memory_space=pltpu.HBM)

COS = (0.99999922, -19.73898252, 64.92872662, -85.27239701, 58.79403871, -21.07678212)
SIN = (6.28318282, -41.3414214, 81.59618388, -76.58010057, 41.20539503, -12.27126259)

NODES = 0.5 - 0.5 * np.cos(np.pi * (2.0 * np.arange(8) + 1.0) / 16.0)
Z = [float(node) for node in NODES]


def lagrange_table(half_cell):
    target = (NODES + half_cell) / 2.0
    table = np.ones((8, 8))
    for s in range(8):
        for n in range(8):
            if n != s:
                table[:, s] *= (target - NODES[n]) / (NODES[s] - NODES[n])
    return table


HALVES = [lagrange_table(0.0), lagrange_table(1.0)]
V = [np.kron(HALVES[u % 2], HALVES[u // 2]) for u in range(4)]
MERGE = np.concatenate([table.T for table in V], axis=1)
SPREAD = np.stack([np.concatenate([V[u2] @ V[u1] for u2 in range(4)]) for u1 in range(4)])


def in_two(table, axis=0):
    whole = table.astype(np.float32)
    high = whole.astype(BF16)
    low = (whole - high.astype(np.float32)).astype(BF16)
    return jnp.asarray(np.stack([high, low], axis=axis))


def polynomial(square, terms, scale):
    value = jnp.full_like(square, terms[-1] * scale)
    for term in terms[-2::-1]:
        value = value * square + term * scale
    return value


def fraction(turns):
    return turns - jnp.round(turns)


def cos_sin(turns, scale=1.0):
    part = fraction(turns)
    square = part * part
    return polynomial(square, COS, scale), part * polynomial(square, SIN, scale)


def root(value):
    return value * lax.rsqrt(value)


def speeds(first_cos_sin, second_cos_sin):
    one = (2.0 + first_cos_sin[1] * second_cos_sin[1]) * (1.0 / 16.0)
    two = (2.0 + first_cos_sin[0] * second_cos_sin[0]) * (1.0 / 16.0)
    return one * one, two * two


def lanes():
    return lax.broadcasted_iota(jnp.int32, (8, 128), 1)


def by_sublane(values):
    row = lax.broadcasted_iota(jnp.int32, (8, 128), 0)
    out = jnp.full((8, 128), values[0], F32)
    for index in range(1, 8):
        out = jnp.where(row == index, values[index], out)
    return out


def from_scalars(ref, base, period):
    place = lanes() % period
    out = jnp.full((8, 128), ref[base], jnp.int32)
    for index in range(1, period):
        out = jnp.where(place == index, ref[base + index], out)
    return out


def swap_four(parts, first_lane):
    digit = lax.broadcasted_iota(jnp.int32, parts[0].shape, parts[0].ndim - 1) // first_lane % 4
    out = []
    for target in range(4):
        value = parts[target]
        for index in range(4):
            if index != target:
                moved = pltpu.roll(parts[index], first_lane * (index - target) % 128, value.ndim - 1)
                value = jnp.where(digit == index, moved, value)
        out.append(value)
    return out


def swap_wide(parts):
    lane = lax.broadcasted_iota(jnp.int32, parts[0].shape, 1)
    lower, even = lane < 64, lane // 32 % 2 == 0
    halves = [None] * 4
    for index in range(2):
        a, b = parts[index], parts[index + 2]
        crossed = pltpu.roll(jnp.where(lower, b, a), 64, 1)
        halves[index], halves[index + 2] = jnp.where(lower, a, crossed), jnp.where(lower, crossed, b)
    out = [None] * 4
    for index in (0, 2):
        a, b = halves[index], halves[index + 1]
        out[index] = jnp.where(even, a, pltpu.roll(b, 32, 1))
        out[index + 1] = jnp.where(even, pltpu.roll(a, 96, 1), b)
    return out


def pack_kernel(source, out0, out1, out2, out3, x_ref, held, sems):
    z = lax.axis_index("dev") % 4
    copies = []
    for part in range(2):
        for low in range(2):
            piece = pl.ds(4 * low, 4)
            copies.append(
                pltpu.make_async_copy(source.at[part, piece], x_ref.at[part, piece], sems.at[2 * part + low])
            )
            copies[-1].start()
    for part in range(2):
        for low in range(2):
            copies[2 * part + low].wait()
            for tile in range(8):
                rows = pl.ds(8 * tile, 8)
                group = [x_ref[part, 4 * low + high, rows, :] for high in range(4)]
                for target, value in enumerate(swap_four(group, 8)):
                    held[target, part, low, rows, :] = value
    for distance, out in zip(ORDER, (out0, out1, out2, out3)):
        target = (z + distance) % 4
        out[...] = held[target]


def table_kernel(
    space_hbm, wave_hbm, merge_hbm, spread_hbm,
    ec, es, switch, rc, rs, merge, spread,
    space_ref, wave_ref, first, second, left, right, sems,
):
    group = lax.axis_index("grp")
    device = lax.axis_index("dev")
    copies = [
        pltpu.make_async_copy(space_hbm, space_ref, sems.at[0]),
        pltpu.make_async_copy(wave_hbm, wave_ref, sems.at[1]),
        pltpu.make_async_copy(merge_hbm, merge, sems.at[2]),
        pltpu.make_async_copy(spread_hbm.at[group], spread, sems.at[3]),
    ]
    for copy in copies:
        copy.start()
    for copy in copies[:2]:
        copy.wait()
    z = device % 4
    base = device // 4 * 32
    lane = lanes()
    node = by_sublane(Z)
    u1x, u1y = group % 2, group // 2
    u2 = lane // 32
    u2x, u2y = u2 % 2, u2 // 2

    space = from_scalars(space_ref, base + z * 8, 8)
    wave = from_scalars(wave_ref, base + z * 8, 8)
    space_x, space_y = space // 32, space % 32
    wave_x, wave_y = wave // 16, wave % 16

    for u0 in range(4):
        ix, iy = 2 * space_x + u0 % 2, 2 * space_y + u0 // 2
        fx, fy = ix.astype(F32) + 0.5, iy.astype(F32) + 0.5
        one, two = speeds(cos_sin(fx * 0.125), cos_sin(fy * 0.125))
        for c in range(4):
            kx = wave_x * 8 + u2x * 4 + u1x * 2 + c % 2 - 64
            ky = wave_y * 8 + u2y * 4 + u1y * 2 + c // 2 - 64
            whole = (((2 * ix + 1) * kx + (2 * iy + 1) * ky) & 3).astype(F32) * 0.25
            fkx, fky = kx.astype(F32), ky.astype(F32)
            k2 = (fky + node) * 32.0
            part2 = whole + fy * 0.5 * node
            rad2 = two * (k2 * k2)
            for s1 in range(8):
                k1 = (fkx + Z[s1]) * 32.0
                turns = part2 + fx * (0.5 * Z[s1]) + root(one * (k1 * k1) + rad2)
                cosine, sine = cos_sin(turns)
                ec[u0, c, pl.ds(8 * s1, 8), :] = cosine
                es[u0, c, pl.ds(8 * s1, 8), :] = -sine

    u0 = lane // 8 % 4
    ix, iy = 2 * space_x + u0 % 2, 2 * space_y + u0 // 2
    kx, ky = wave_x * 4 + u2x * 2 + u1x - 32, wave_y * 4 + u2y * 2 + u1y - 32
    fx, fy = ix.astype(F32), iy.astype(F32)
    fkx, fky = kx.astype(F32), ky.astype(F32)
    half_x = ((kx + ix) & 1).astype(F32) * 0.5
    half_y = ((ky + iy) & 1).astype(F32) * 0.5
    one_a, two_a = speeds(cos_sin((fx + 0.5) * 0.125), cos_sin((fy + 0.5) * 0.125))
    turn2 = cos_sin((fy + node) * 0.125)
    squares1, squares2 = [], []
    for s in range(8):
        k1, k2 = (fkx + Z[s]) * 64.0, (fky + Z[s]) * 64.0
        squares1.append(k1 * k1)
        squares2.append(k2 * k2)
    for s1 in range(8):
        for s2 in range(8):
            linear = (2.0 * fy + 0.5) * Z[s2] + node * (Z[s2] - 0.5) + half_y
            right[s1, s2] = fraction(linear + root(one_a * squares1[s1] + two_a * squares2[s2]))
    b1, b2 = (fkx + 0.5) * 64.0, (fky + 0.5) * 64.0
    for t1 in range(8):
        one, two = speeds(cos_sin((fx + Z[t1]) * 0.125), turn2)
        back = root(one * (b1 * b1) + two * (b2 * b2))
        for s in range(8):
            linear = (2.0 * fx + 0.5) * Z[s] + (Z[t1] * (Z[s] - 0.5)) + half_x
            left[t1, s] = fraction(linear - back)
            first[t1, s] = one * squares1[s]
            second[t1, s] = two * squares2[s]

    def switch_rows(s1, _):
        for s2 in range(8):
            cosines, sines = [], []
            for t1 in range(8):
                turns = left[t1, s1] + right[s1, s2] + root(first[t1, s1] + second[t1, s2])
                cosine, sine = cos_sin(turns, 1.0 / 64.0)
                cosines.append(cosine)
                sines.append(sine)
            turned = jnp.concatenate(cosines + sines).T
            for tile in range(16):
                switch[pl.ds(tile * 8 * PITCH + s1 * 8 + s2, 8, stride=PITCH), :] = turned[8 * tile : 8 * tile + 8]
        return 0

    lax.fori_loop(0, 8, switch_rows, 0)

    space = from_scalars(space_ref, base, 32)
    wave = from_scalars(wave_ref, base, 32)
    ix, iy = space // 32, space % 32
    for bit_x, bit_y in ((z % 2, z // 2), (u1x, u1y), (u2x, u2y)):
        ix, iy = 2 * ix + bit_x, 2 * iy + bit_y
    fx, fy = ix.astype(F32), iy.astype(F32)
    fkx = (wave // 16 - 8).astype(F32) + 0.5
    fky = (wave % 16 - 8).astype(F32) + 0.5
    halves = ((ix + iy) & 1).astype(F32) * 0.5
    turn2 = cos_sin((fy + node) * 0.03125)
    b1, b2 = fkx * 256.0, fky * 256.0
    for t1 in range(8):
        one, two = speeds(cos_sin((fx + Z[t1]) * 0.03125), turn2)
        turns = halves + fkx * Z[t1] + fky * node + root(one * (b1 * b1) + two * (b2 * b2))
        cosine, sine = cos_sin(turns)
        rc[pl.ds(8 * t1, 8), :] = cosine
        rs[pl.ds(8 * t1, 8), :] = sine
    for copy in copies[2:]:
        copy.wait()


def split(value):
    high = value.astype(BF16)
    return high, (value - high.astype(F32)).astype(BF16)


def dot(a, b):
    return jnp.dot(a, b, preferred_element_type=F32)


def main_kernel(y0, y1, y2, y3, ec, es, switch, merge, out, turned_high, turned_low, turned, sums):
    z = lax.axis_index("dev") % 4
    for u0 in range(4):
        for distance, y in zip(ORDER, (y0, y1, y2, y3)):
            child = (z + 4 - distance) % 4
            start = pl.multiple_of(child * 64, 64)
            for half in range(4):
                spot = pl.ds(16 * half, 16)
                cosine, sine = ec[u0, child, spot, :], es[u0, child, spot, :]
                for low in range(2):
                    re, im = y[0, low, spot, :], y[1, low, spot, :]
                    for part, value in enumerate((re * cosine - im * sine, re * sine + im * cosine)):
                        high, rest = split(value)
                        columns = pl.ds((2 * part + low) * 128, 128)
                        turned_high[pl.ds(start + 16 * half, 16), columns] = high
                        turned_low[pl.ds(start + 16 * half, 16), columns] = rest
        product = dot(merge[...], turned_high[...])
        summed = product[:64] + product[64:] + dot(merge[:64], turned_low[...])
        for low in range(2):
            re, im = summed[:, low * 128 : low * 128 + 128], summed[:, (2 + low) * 128 : (2 + low) * 128 + 128]
            flat = jnp.concatenate([re, im]).T
            for u2 in range(4):
                for high in range(4):
                    start = (u2 * 32 + u0 * 8) * 8 + low * 4 + high
                    tile = (u2 * 4 + high) * 8
                    turned[pl.ds(start, 8, stride=8), :] = flat[tile : tile + 8]

    lane = lanes()
    left = lane < 64
    for u0 in range(4):
        for r in range(8):
            pair = [u2 * 32 + u0 * 8 + r for u2 in range(4)]
            value = [turned[pl.ds(8 * m, 8), :] for m in pair]
            other = [pltpu.roll(v, 64, 1) for v in value]
            re = [jnp.where(left, value[u], other[u + 1]) for u in (0, 2)]
            im = [jnp.where(left, other[u], value[u + 1]) for u in (0, 2)]
            high, low = split(jnp.concatenate([jnp.concatenate(re, axis=1), jnp.concatenate(im, axis=1)]))
            matrix_high, matrix_low = split(jnp.concatenate([switch[pl.ds(PITCH * m, 64), :] for m in pair]))
            product = dot(jnp.concatenate([high, low]), matrix_high)
            product = product[:16] + product[16:] + dot(high, matrix_low)
            crossed = pltpu.roll(product[8:], 64, 1)
            total = product[:8] + jnp.where(left, -crossed, crossed)
            sums[u0, pl.ds(r, 8, stride=8), :] = total
            sums[u0, pl.ds(64 + r, 8, stride=8), :] = pltpu.roll(total, 64, 1)
    for u0 in range(4):
        out[u0] = sums[u0].T[:64]


def sum_kernel(own, other, out0, out1, out2, out3):
    z = lax.axis_index("dev") % 4
    for distance, out in zip(ORDER, (out0, out1, out2, out3)):
        target = (z + distance) % 4
        out[...] = own[target] + other[target]


def last_kernel(r0, r1, r2, r3, spread, rc, rs, target, held, high_ref, low_ref, spreaded, out, sems):
    z = lax.axis_index("dev") % 4
    for distance, r in zip(ORDER, (r0, r1, r2, r3)):
        held[(z + 4 - distance) % 4] = r[...]
    for tile in range(4):
        spot = pl.ds(16 * tile, 16)
        for low, value in enumerate(swap_four([held[source, spot, :] for source in range(4)], 8)):
            high, rest = split(value)
            high_ref[low, spot, :] = high
            low_ref[low, spot, :] = rest
    for low in range(4):
        spreaded[low] = (
            dot(spread[0], high_ref[low]) + dot(spread[0], low_ref[low]) + dot(spread[1], high_ref[low])
        )
    copies = []
    for tile in range(8):
        entry = [None] * 16
        for low in range(4):
            parts = [spreaded[low, pl.ds(64 * u2 + 8 * tile, 8), :] for u2 in range(4)]
            for high, value in enumerate(swap_wide(parts)):
                entry[4 * high + low] = value
        spot = pl.ds(8 * tile, 8)
        cosine, sine = rc[spot, :], rs[spot, :]
        for k in range(8):
            re, im = entry[k], entry[8 + k]
            out[0, k, spot, :] = re * cosine - im * sine
            out[1, k, spot, :] = re * sine + im * cosine
        if tile % 2:
            rows = pl.ds(8 * tile - 8, 16)
            copies.append(pltpu.make_async_copy(out.at[:, :, rows, :], target.at[:, :, rows, :], sems.at[tile // 2]))
            copies[-1].start()
    for copy in copies:
        copy.wait()


def call(kernel, inputs, outs, scratch=(), flops=0, place=VMEM):
    return pl.pallas_call(
        kernel,
        out_shape=outs,
        in_specs=[spec for spec, _ in inputs],
        out_specs=jax.tree.map(lambda _: place, outs),
        scratch_shapes=scratch,
        cost_estimate=pl.CostEstimate(flops=flops, bytes_accessed=1 << 20, transcendentals=0),
        compiler_params=pltpu.CompilerParams(vmem_limit_bytes=40 << 20),
    )(*[value for _, value in inputs])


def in_hbm(value):
    return pltpu.with_memory_space_constraint(value, pltpu.HBM)


def shape(*dims, kind=F32):
    return jax.ShapeDtypeStruct(dims, kind)


def along_z(value, distance):
    route = [(low, low // 4 * 4 + (low + distance) % 4) for low in range(lax.axis_size("dev"))]
    return lax.ppermute(value, "dev", route)


def exchange(pieces):
    return [along_z(piece, distance) if distance else piece for distance, piece in zip(ORDER, pieces)]


def across_groups(value, bit):
    return lax.ppermute(value, "grp", [(low, low ^ bit) for low in range(4)])


def per_device(coefficients, spatial_root, frequency_root):
    packed = call(
        pack_kernel,
        [(HBM, in_hbm(coefficients))],
        [shape(2, 2, 64, 128)] * 4,
        [pltpu.VMEM((2, 8, 64, 128), F32), pltpu.VMEM((4, 2, 2, 64, 128), F32), pltpu.SemaphoreType.DMA((4,))],
        flops=1 << 20,
    )
    arrived = exchange(packed)
    tables = call(
        table_kernel,
        [(HBM, in_hbm(value)) for value in (spatial_root, frequency_root, in_two(MERGE).reshape(128, 256), in_two(SPREAD, 1))],
        [shape(4, 4, 64, 128)] * 2
        + [shape(128 * PITCH, 128)]
        + [shape(64, 128)] * 2
        + [shape(128, 256, kind=BF16), shape(2, 256, 64, kind=BF16)],
        [pltpu.SMEM((256,), jnp.int32)] * 2
        + [pltpu.VMEM((8, 8, 8, 128), F32)] * 4
        + [pltpu.SemaphoreType.DMA((4,))],
        flops=1 << 26,
    )
    ec, es, switch, rc, rs, merge, spread = tables
    partial = call(
        main_kernel,
        [(VMEM, value) for value in (*arrived, ec, es, switch, merge)],
        shape(4, 64, 128),
        [
            pltpu.VMEM((256, 512), BF16),
            pltpu.VMEM((256, 512), BF16),
            pltpu.VMEM((1024, 128), F32),
            pltpu.VMEM((4, 128, 128), F32),
        ],
        flops=1 << 27,
    )
    partial = partial + across_groups(partial, 1)
    summed = call(
        sum_kernel,
        [(VMEM, partial), (VMEM, across_groups(partial, 2))],
        [shape(64, 128)] * 4,
        flops=1 << 18,
    )
    blocks = exchange(summed)
    return call(
        last_kernel,
        [(VMEM, value) for value in (*blocks, spread, rc, rs)],
        shape(2, 8, 64, 128),
        [
            pltpu.VMEM((4, 64, 128), F32),
            pltpu.VMEM((4, 64, 128), BF16),
            pltpu.VMEM((4, 64, 128), BF16),
            pltpu.VMEM((4, 256, 128), F32),
            pltpu.VMEM((2, 8, 64, 128), F32),
            pltpu.SemaphoreType.DMA((4,)),
        ],
        flops=1 << 24,
        place=HBM,
    )


def solution(mesh):
    return jax.shard_map(
        per_device,
        mesh=mesh,
        in_specs=(P(None, None, None, ("grp", "dev")), P(), P()),
        out_specs=P(None, None, None, ("grp", "dev")),
        check_vma=False,
    )
```

```python
import functools

import jax
import jax.numpy as jnp
import numpy as np
from jax import lax
from jax.experimental import pallas as pl
from jax.experimental.pallas import tpu as pltpu
from jax.sharding import PartitionSpec as P


F32 = jnp.float32
PITCH = 72
ORDER = (2, 1, 3, 0)
BF16 = jnp.bfloat16
VMEM = pl.BlockSpec(memory_space=pltpu.VMEM)
HBM = pl.BlockSpec(memory_space=pltpu.HBM)

COS = (0.99999922, -19.73898252, 64.92872662, -85.27239701, 58.79403871, -21.07678212)
SIN = (6.28318282, -41.3414214, 81.59618388, -76.58010057, 41.20539503, -12.27126259)

NODES = 0.5 - 0.5 * np.cos(np.pi * (2.0 * np.arange(8) + 1.0) / 16.0)
Z = [float(node) for node in NODES]


def lagrange_table(half_cell):
    target = (NODES + half_cell) / 2.0
    table = np.ones((8, 8))
    for s in range(8):
        for n in range(8):
            if n != s:
                table[:, s] *= (target - NODES[n]) / (NODES[s] - NODES[n])
    return table


HALVES = [lagrange_table(0.0), lagrange_table(1.0)]
V = [np.kron(HALVES[u % 2], HALVES[u // 2]) for u in range(4)]
MERGE = np.concatenate([table.T for table in V], axis=1)
SPREAD = np.stack([np.concatenate([V[u2] @ V[u1] for u2 in range(4)]) for u1 in range(4)])


def in_two(table, axis=0):
    whole = table.astype(np.float32)
    high = whole.astype(BF16)
    low = (whole - high.astype(np.float32)).astype(BF16)
    return jnp.asarray(np.stack([high, low], axis=axis))


def polynomial(square, terms, scale):
    value = jnp.full_like(square, terms[-1] * scale)
    for term in terms[-2::-1]:
        value = value * square + term * scale
    return value


def fraction(turns):
    return turns - jnp.round(turns)


def cos_sin(turns, scale=1.0):
    part = fraction(turns)
    square = part * part
    return polynomial(square, COS, scale), part * polynomial(square, SIN, scale)


def root(value):
    return value * lax.rsqrt(value)


def speeds(first_cos_sin, second_cos_sin):
    one = (2.0 + first_cos_sin[1] * second_cos_sin[1]) * (1.0 / 16.0)
    two = (2.0 + first_cos_sin[0] * second_cos_sin[0]) * (1.0 / 16.0)
    return one * one, two * two


def lanes():
    return lax.broadcasted_iota(jnp.int32, (8, 128), 1)


def by_sublane(values):
    row = lax.broadcasted_iota(jnp.int32, (8, 128), 0)
    out = jnp.full((8, 128), values[0], F32)
    for index in range(1, 8):
        out = jnp.where(row == index, values[index], out)
    return out


def from_scalars(ref, base, period):
    place = lanes() % period
    out = jnp.full((8, 128), ref[base], jnp.int32)
    for index in range(1, period):
        out = jnp.where(place == index, ref[base + index], out)
    return out


def swap_four(parts, first_lane):
    digit = lax.broadcasted_iota(jnp.int32, parts[0].shape, parts[0].ndim - 1) // first_lane % 4
    out = []
    for target in range(4):
        value = parts[target]
        for index in range(4):
            if index != target:
                moved = pltpu.roll(parts[index], first_lane * (index - target) % 128, value.ndim - 1)
                value = jnp.where(digit == index, moved, value)
        out.append(value)
    return out


def swap_wide(parts):
    lane = lax.broadcasted_iota(jnp.int32, parts[0].shape, 1)
    lower, even = lane < 64, lane // 32 % 2 == 0
    halves = [None] * 4
    for index in range(2):
        a, b = parts[index], parts[index + 2]
        crossed = pltpu.roll(jnp.where(lower, b, a), 64, 1)
        halves[index], halves[index + 2] = jnp.where(lower, a, crossed), jnp.where(lower, crossed, b)
    out = [None] * 4
    for index in (0, 2):
        a, b = halves[index], halves[index + 1]
        out[index] = jnp.where(even, a, pltpu.roll(b, 32, 1))
        out[index + 1] = jnp.where(even, pltpu.roll(a, 96, 1), b)
    return out


def pack_piece(x_ref, part, low, tile, target):
    rows = pl.ds(8 * tile, 8)
    digit = lanes() // 8 % 4
    value = None
    for high in range(4):
        shift = 8 * ((high + 16 - target) % 16)
        moved = pltpu.roll(x_ref[part, 4 * low + high, rows, :], shift, 1)
        value = moved if value is None else jnp.where(digit == high, moved, value)
    return value


def pack_far_kernel(source, out, x_ref, sems):
    z = lax.axis_index("dev") % 4
    copies = []
    for part in range(2):
        for low in range(2):
            piece = pl.ds(4 * low, 4)
            copies.append(
                pltpu.make_async_copy(source.at[part, piece], x_ref.at[part, piece], sems.at[2 * part + low])
            )
            copies[-1].start()
    for part in range(2):
        for low in range(2):
            copies[2 * part + low].wait()
            for tile in range(8):
                out[part, low, pl.ds(8 * tile, 8), :] = pack_piece(x_ref, part, low, tile, (z + ORDER[0]) % 4)


def pack_near_kernel(x_ref, out0, out1, out2):
    z = lax.axis_index("dev") % 4
    for part in range(2):
        for low in range(2):
            for tile in range(8):
                for distance, out in zip(ORDER[1:], (out0, out1, out2)):
                    out[part, low, pl.ds(8 * tile, 8), :] = pack_piece(x_ref, part, low, tile, (z + distance) % 4)


def table_kernel(
    space_hbm, wave_hbm, merge_hbm, spread_hbm,
    ec, es, switch, rc, rs, merge, spread,
    space_ref, wave_ref, first, second, left, right, sems,
):
    group = lax.axis_index("grp")
    device = lax.axis_index("dev")
    copies = [
        pltpu.make_async_copy(space_hbm, space_ref, sems.at[0]),
        pltpu.make_async_copy(wave_hbm, wave_ref, sems.at[1]),
        pltpu.make_async_copy(merge_hbm, merge, sems.at[2]),
        pltpu.make_async_copy(spread_hbm.at[group], spread, sems.at[3]),
    ]
    for copy in copies:
        copy.start()
    for copy in copies[:2]:
        copy.wait()
    z = device % 4
    base = device // 4 * 32
    lane = lanes()
    node = by_sublane(Z)
    u1x, u1y = group % 2, group // 2
    u2 = lane // 32
    u2x, u2y = u2 % 2, u2 // 2

    space = from_scalars(space_ref, base + z * 8, 8)
    wave = from_scalars(wave_ref, base + z * 8, 8)
    space_x, space_y = space // 32, space % 32
    wave_x, wave_y = wave // 16, wave % 16

    for u0 in range(4):
        ix, iy = 2 * space_x + u0 % 2, 2 * space_y + u0 // 2
        fx, fy = ix.astype(F32) + 0.5, iy.astype(F32) + 0.5
        one, two = speeds(cos_sin(fx * 0.125), cos_sin(fy * 0.125))
        for c in range(4):
            kx = wave_x * 8 + u2x * 4 + u1x * 2 + c % 2 - 64
            ky = wave_y * 8 + u2y * 4 + u1y * 2 + c // 2 - 64
            whole = (((2 * ix + 1) * kx + (2 * iy + 1) * ky) & 3).astype(F32) * 0.25
            fkx, fky = kx.astype(F32), ky.astype(F32)
            k2 = (fky + node) * 32.0
            part2 = whole + fy * 0.5 * node
            rad2 = two * (k2 * k2)
            for s1 in range(8):
                k1 = (fkx + Z[s1]) * 32.0
                turns = part2 + fx * (0.5 * Z[s1]) + root(one * (k1 * k1) + rad2)
                cosine, sine = cos_sin(turns)
                ec[u0, c, pl.ds(8 * s1, 8), :] = cosine
                es[u0, c, pl.ds(8 * s1, 8), :] = -sine

    u0 = lane // 8 % 4
    ix, iy = 2 * space_x + u0 % 2, 2 * space_y + u0 // 2
    kx, ky = wave_x * 4 + u2x * 2 + u1x - 32, wave_y * 4 + u2y * 2 + u1y - 32
    fx, fy = ix.astype(F32), iy.astype(F32)
    fkx, fky = kx.astype(F32), ky.astype(F32)
    half_x = ((kx + ix) & 1).astype(F32) * 0.5
    half_y = ((ky + iy) & 1).astype(F32) * 0.5
    one_a, two_a = speeds(cos_sin((fx + 0.5) * 0.125), cos_sin((fy + 0.5) * 0.125))
    turn2 = cos_sin((fy + node) * 0.125)
    squares1, squares2 = [], []
    for s in range(8):
        k1, k2 = (fkx + Z[s]) * 64.0, (fky + Z[s]) * 64.0
        squares1.append(k1 * k1)
        squares2.append(k2 * k2)
    for s1 in range(8):
        for s2 in range(8):
            linear = (2.0 * fy + 0.5) * Z[s2] + node * (Z[s2] - 0.5) + half_y
            right[s1, s2] = fraction(linear + root(one_a * squares1[s1] + two_a * squares2[s2]))
    b1, b2 = (fkx + 0.5) * 64.0, (fky + 0.5) * 64.0
    for t1 in range(8):
        one, two = speeds(cos_sin((fx + Z[t1]) * 0.125), turn2)
        back = root(one * (b1 * b1) + two * (b2 * b2))
        for s in range(8):
            linear = (2.0 * fx + 0.5) * Z[s] + (Z[t1] * (Z[s] - 0.5)) + half_x
            left[t1, s] = fraction(linear - back)
            first[t1, s] = one * squares1[s]
            second[t1, s] = two * squares2[s]

    def switch_rows(s1, _):
        for s2 in range(8):
            cosines, sines = [], []
            for t1 in range(8):
                turns = left[t1, s1] + right[s1, s2] + root(first[t1, s1] + second[t1, s2])
                cosine, sine = cos_sin(turns, 1.0 / 64.0)
                cosines.append(cosine)
                sines.append(sine)
            turned = jnp.concatenate(cosines + sines).T
            for tile in range(16):
                switch[pl.ds(tile * 8 * PITCH + s1 * 8 + s2, 8, stride=PITCH), :] = turned[8 * tile : 8 * tile + 8]
        return 0

    lax.fori_loop(0, 8, switch_rows, 0)

    space = from_scalars(space_ref, base, 32)
    wave = from_scalars(wave_ref, base, 32)
    ix, iy = space // 32, space % 32
    for bit_x, bit_y in ((z % 2, z // 2), (u1x, u1y), (u2x, u2y)):
        ix, iy = 2 * ix + bit_x, 2 * iy + bit_y
    fx, fy = ix.astype(F32), iy.astype(F32)
    fkx = (wave // 16 - 8).astype(F32) + 0.5
    fky = (wave % 16 - 8).astype(F32) + 0.5
    halves = ((ix + iy) & 1).astype(F32) * 0.5
    turn2 = cos_sin((fy + node) * 0.03125)
    b1, b2 = fkx * 256.0, fky * 256.0
    for t1 in range(8):
        one, two = speeds(cos_sin((fx + Z[t1]) * 0.03125), turn2)
        turns = halves + fkx * Z[t1] + fky * node + root(one * (b1 * b1) + two * (b2 * b2))
        cosine, sine = cos_sin(turns)
        rc[pl.ds(8 * t1, 8), :] = cosine
        rs[pl.ds(8 * t1, 8), :] = sine
    for copy in copies[2:]:
        copy.wait()


def split(value):
    high = value.astype(BF16)
    return high, (value - high.astype(F32)).astype(BF16)


def dot(a, b):
    return jnp.dot(a, b, preferred_element_type=F32)


def main_kernel(y0, y1, y2, y3, ec, es, switch, merge, out, turned_high, turned_low, turned, sums):
    z = lax.axis_index("dev") % 4
    for u0 in range(4):
        for distance, y in zip(ORDER, (y0, y1, y2, y3)):
            child = (z + 4 - distance) % 4
            start = pl.multiple_of(child * 64, 64)
            for half in range(4):
                spot = pl.ds(16 * half, 16)
                cosine, sine = ec[u0, child, spot, :], es[u0, child, spot, :]
                for low in range(2):
                    re, im = y[0, low, spot, :], y[1, low, spot, :]
                    for part, value in enumerate((re * cosine - im * sine, re * sine + im * cosine)):
                        high, rest = split(value)
                        columns = pl.ds((2 * part + low) * 128, 128)
                        turned_high[pl.ds(start + 16 * half, 16), columns] = high
                        turned_low[pl.ds(start + 16 * half, 16), columns] = rest
        product = dot(merge[...], turned_high[...])
        summed = product[:64] + product[64:] + dot(merge[:64], turned_low[...])
        for low in range(2):
            re, im = summed[:, low * 128 : low * 128 + 128], summed[:, (2 + low) * 128 : (2 + low) * 128 + 128]
            flat = jnp.concatenate([re, im]).T
            for u2 in range(4):
                for high in range(4):
                    start = (u2 * 32 + u0 * 8) * 8 + low * 4 + high
                    tile = (u2 * 4 + high) * 8
                    turned[pl.ds(start, 8, stride=8), :] = flat[tile : tile + 8]

    lane = lanes()
    left = lane < 64
    for u0 in range(4):
        for r in range(8):
            pair = [u2 * 32 + u0 * 8 + r for u2 in range(4)]
            value = [turned[pl.ds(8 * m, 8), :] for m in pair]
            other = [pltpu.roll(v, 64, 1) for v in value]
            re = [jnp.where(left, value[u], other[u + 1]) for u in (0, 2)]
            im = [jnp.where(left, other[u], value[u + 1]) for u in (0, 2)]
            high, low = split(jnp.concatenate([jnp.concatenate(re, axis=1), jnp.concatenate(im, axis=1)]))
            matrix_high, matrix_low = split(jnp.concatenate([switch[pl.ds(PITCH * m, 64), :] for m in pair]))
            product = dot(jnp.concatenate([high, low]), matrix_high)
            product = product[:16] + product[16:] + dot(high, matrix_low)
            crossed = pltpu.roll(product[8:], 64, 1)
            total = product[:8] + jnp.where(left, -crossed, crossed)
            sums[u0, pl.ds(r, 8, stride=8), :] = total
            sums[u0, pl.ds(64 + r, 8, stride=8), :] = pltpu.roll(total, 64, 1)
    for u0 in range(4):
        out[u0] = sums[u0].T[:64]


def sum_kernel(own, other, out0, out1, out2, out3):
    z = lax.axis_index("dev") % 4
    for distance, out in zip(ORDER, (out0, out1, out2, out3)):
        target = (z + distance) % 4
        out[...] = own[target] + other[target]


def last_kernel(r0, r1, r2, r3, spread, rc, rs, target, held, high_ref, low_ref, spreaded, out, sems):
    z = lax.axis_index("dev") % 4
    for distance, r in zip(ORDER, (r0, r1, r2, r3)):
        held[(z + 4 - distance) % 4] = r[...]
    for tile in range(4):
        spot = pl.ds(16 * tile, 16)
        for low, value in enumerate(swap_four([held[source, spot, :] for source in range(4)], 8)):
            high, rest = split(value)
            high_ref[low, spot, :] = high
            low_ref[low, spot, :] = rest
    for low in range(4):
        spreaded[low] = (
            dot(spread[0], high_ref[low]) + dot(spread[0], low_ref[low]) + dot(spread[1], high_ref[low])
        )
    copies = []
    for tile in range(8):
        entry = [None] * 16
        for low in range(4):
            parts = [spreaded[low, pl.ds(64 * u2 + 8 * tile, 8), :] for u2 in range(4)]
            for high, value in enumerate(swap_wide(parts)):
                entry[4 * high + low] = value
        spot = pl.ds(8 * tile, 8)
        cosine, sine = rc[spot, :], rs[spot, :]
        for k in range(8):
            re, im = entry[k], entry[8 + k]
            out[0, k, spot, :] = re * cosine - im * sine
            out[1, k, spot, :] = re * sine + im * cosine
        if tile % 2:
            rows = pl.ds(8 * tile - 8, 16)
            copies.append(pltpu.make_async_copy(out.at[:, :, rows, :], target.at[:, :, rows, :], sems.at[tile // 2]))
            copies[-1].start()
    for copy in copies:
        copy.wait()


def call(kernel, inputs, outs, scratch=(), flops=0, place=VMEM):
    return pl.pallas_call(
        kernel,
        out_shape=outs,
        in_specs=[spec for spec, _ in inputs],
        out_specs=jax.tree.map(lambda _: place, outs),
        scratch_shapes=scratch,
        cost_estimate=pl.CostEstimate(flops=flops, bytes_accessed=1 << 20, transcendentals=0),
        compiler_params=pltpu.CompilerParams(vmem_limit_bytes=40 << 20),
    )(*[value for _, value in inputs])


def in_hbm(value):
    return pltpu.with_memory_space_constraint(value, pltpu.HBM)


def shape(*dims, kind=F32):
    return jax.ShapeDtypeStruct(dims, kind)


def along_z(value, distance):
    route = [(low, low // 4 * 4 + (low + distance) % 4) for low in range(lax.axis_size("dev"))]
    return lax.ppermute(value, "dev", route)


def across_groups(value, bit):
    return lax.ppermute(value, "grp", [(low, low ^ bit) for low in range(4)])


def per_device(coefficients, spatial_root, frequency_root):
    far, held = call(
        pack_far_kernel,
        [(HBM, in_hbm(coefficients))],
        [shape(2, 2, 64, 128), shape(2, 8, 64, 128)],
        [pltpu.SemaphoreType.DMA((4,))],
        flops=1 << 20,
    )
    arrived = [along_z(far, ORDER[0])]
    near = call(pack_near_kernel, [(VMEM, held)], [shape(2, 2, 64, 128)] * 3, flops=1 << 20)
    arrived += [along_z(near[0], ORDER[1]), along_z(near[1], ORDER[2]), near[2]]
    tables = call(
        table_kernel,
        [(HBM, in_hbm(value)) for value in (spatial_root, frequency_root, in_two(MERGE).reshape(128, 256), in_two(SPREAD, 1))],
        [shape(4, 4, 64, 128)] * 2
        + [shape(128 * PITCH, 128)]
        + [shape(64, 128)] * 2
        + [shape(128, 256, kind=BF16), shape(2, 256, 64, kind=BF16)],
        [pltpu.SMEM((256,), jnp.int32)] * 2
        + [pltpu.VMEM((8, 8, 8, 128), F32)] * 4
        + [pltpu.SemaphoreType.DMA((4,))],
        flops=1 << 26,
    )
    ec, es, switch, rc, rs, merge, spread = tables
    partial = call(
        main_kernel,
        [(VMEM, value) for value in (*arrived, ec, es, switch, merge)],
        shape(4, 64, 128),
        [
            pltpu.VMEM((256, 512), BF16),
            pltpu.VMEM((256, 512), BF16),
            pltpu.VMEM((1024, 128), F32),
            pltpu.VMEM((4, 128, 128), F32),
        ],
        flops=1 << 27,
    )
    partial = partial + across_groups(partial, 1)
    summed = call(
        sum_kernel,
        [(VMEM, partial), (VMEM, across_groups(partial, 2))],
        [shape(64, 128)] * 4,
        flops=1 << 18,
    )
    blocks = [along_z(piece, distance) if distance else piece for distance, piece in zip(ORDER, summed)]
    return call(
        last_kernel,
        [(VMEM, value) for value in (*blocks, spread, rc, rs)],
        shape(2, 8, 64, 128),
        [
            pltpu.VMEM((4, 64, 128), F32),
            pltpu.VMEM((4, 64, 128), BF16),
            pltpu.VMEM((4, 64, 128), BF16),
            pltpu.VMEM((4, 256, 128), F32),
            pltpu.VMEM((2, 8, 64, 128), F32),
            pltpu.SemaphoreType.DMA((4,)),
        ],
        flops=1 << 24,
        place=HBM,
    )


def solution(mesh):
    return jax.shard_map(
        per_device,
        mesh=mesh,
        in_specs=(P(None, None, None, ("grp", "dev")), P(), P()),
        out_specs=P(None, None, None, ("grp", "dev")),
        check_vma=False,
    )
```

```python
import functools

import jax
import jax.numpy as jnp
import numpy as np
from jax import lax
from jax.experimental import pallas as pl
from jax.experimental.pallas import tpu as pltpu
from jax.sharding import PartitionSpec as P


F32 = jnp.float32
PITCH = 72
ORDER = (2, 3, 1, 0)
BACK = (2, 1, 3, 0)
BF16 = jnp.bfloat16
VMEM = pl.BlockSpec(memory_space=pltpu.VMEM)
HBM = pl.BlockSpec(memory_space=pltpu.HBM)

COS = (0.99999922, -19.73898252, 64.92872662, -85.27239701, 58.79403871, -21.07678212)
SIN = (6.28318282, -41.3414214, 81.59618388, -76.58010057, 41.20539503, -12.27126259)

NODES = 0.5 - 0.5 * np.cos(np.pi * (2.0 * np.arange(8) + 1.0) / 16.0)
Z = [float(node) for node in NODES]


def lagrange_table(half_cell):
    target = (NODES + half_cell) / 2.0
    table = np.ones((8, 8))
    for s in range(8):
        for n in range(8):
            if n != s:
                table[:, s] *= (target - NODES[n]) / (NODES[s] - NODES[n])
    return table


HALVES = [lagrange_table(0.0), lagrange_table(1.0)]
V = [np.kron(HALVES[u % 2], HALVES[u // 2]) for u in range(4)]
MERGE = np.concatenate([table.T for table in V], axis=1)
SPREAD = np.stack([np.concatenate([V[u2] @ V[u1] for u2 in range(4)]) for u1 in range(4)])


def in_two(table, axis=0):
    whole = table.astype(np.float32)
    high = whole.astype(BF16)
    low = (whole - high.astype(np.float32)).astype(BF16)
    return jnp.asarray(np.stack([high, low], axis=axis))


def polynomial(square, terms, scale):
    value = jnp.full_like(square, terms[-1] * scale)
    for term in terms[-2::-1]:
        value = value * square + term * scale
    return value


def fraction(turns):
    return turns - jnp.round(turns)


def cos_sin(turns, scale=1.0):
    part = fraction(turns)
    square = part * part
    return polynomial(square, COS, scale), part * polynomial(square, SIN, scale)


def root(value):
    return value * lax.rsqrt(value)


def speeds(first_cos_sin, second_cos_sin):
    one = (2.0 + first_cos_sin[1] * second_cos_sin[1]) * (1.0 / 16.0)
    two = (2.0 + first_cos_sin[0] * second_cos_sin[0]) * (1.0 / 16.0)
    return one * one, two * two


def lanes():
    return lax.broadcasted_iota(jnp.int32, (8, 128), 1)


def by_sublane(values):
    row = lax.broadcasted_iota(jnp.int32, (8, 128), 0)
    out = jnp.full((8, 128), values[0], F32)
    for index in range(1, 8):
        out = jnp.where(row == index, values[index], out)
    return out


def from_scalars(ref, base, period):
    place = lanes() % period
    out = jnp.full((8, 128), ref[base], jnp.int32)
    for index in range(1, period):
        out = jnp.where(place == index, ref[base + index], out)
    return out


def swap_four(parts, first_lane):
    digit = lax.broadcasted_iota(jnp.int32, parts[0].shape, parts[0].ndim - 1) // first_lane % 4
    out = []
    for target in range(4):
        value = parts[target]
        for index in range(4):
            if index != target:
                moved = pltpu.roll(parts[index], first_lane * (index - target) % 128, value.ndim - 1)
                value = jnp.where(digit == index, moved, value)
        out.append(value)
    return out


def swap_wide(parts):
    lane = lax.broadcasted_iota(jnp.int32, parts[0].shape, 1)
    lower, even = lane < 64, lane // 32 % 2 == 0
    halves = [None] * 4
    for index in range(2):
        a, b = parts[index], parts[index + 2]
        crossed = pltpu.roll(jnp.where(lower, b, a), 64, 1)
        halves[index], halves[index + 2] = jnp.where(lower, a, crossed), jnp.where(lower, crossed, b)
    out = [None] * 4
    for index in (0, 2):
        a, b = halves[index], halves[index + 1]
        out[index] = jnp.where(even, a, pltpu.roll(b, 32, 1))
        out[index + 1] = jnp.where(even, pltpu.roll(a, 96, 1), b)
    return out


def pack_piece(x_ref, part, low, tile, target):
    rows = pl.ds(8 * tile, 8)
    digit = lanes() // 8 % 4
    value = None
    for high in range(4):
        shift = 8 * ((high + 16 - target) % 16)
        moved = pltpu.roll(x_ref[part, 4 * low + high, rows, :], shift, 1)
        value = moved if value is None else jnp.where(digit == high, moved, value)
    return value


def pack_far_kernel(source, space_hbm, wave_hbm, out, x_ref, box, space_ref, wave_ref, sems):
    device = lax.axis_index("dev")
    z = device % 4
    base = device // 4 * 32
    roots = [
        pltpu.make_async_copy(space_hbm, space_ref, sems.at[4]),
        pltpu.make_async_copy(wave_hbm, wave_ref, sems.at[5]),
    ]
    for copy in roots:
        copy.start()
    copies = []
    for part in range(2):
        for low in range(2):
            piece = pl.ds(4 * low, 4)
            copies.append(
                pltpu.make_async_copy(source.at[part, piece], x_ref.at[part, piece], sems.at[2 * part + low])
            )
            copies[-1].start()
    for copy in roots:
        copy.wait()
    box[0] = from_scalars(space_ref, base + z * 8, 8)
    box[1] = from_scalars(wave_ref, base + z * 8, 8)
    box[2] = from_scalars(space_ref, base, 32)
    box[3] = from_scalars(wave_ref, base, 32)
    for part in range(2):
        for low in range(2):
            copies[2 * part + low].wait()
            for tile in range(8):
                out[part, low, pl.ds(8 * tile, 8), :] = pack_piece(x_ref, part, low, tile, (z + ORDER[0]) % 4)


def pack_near_kernel(x_ref, out0, out1, out2):
    z = lax.axis_index("dev") % 4
    for part in range(2):
        for low in range(2):
            for tile in range(8):
                for distance, out in zip(ORDER[1:], (out0, out1, out2)):
                    out[part, low, pl.ds(8 * tile, 8), :] = pack_piece(x_ref, part, low, tile, (z + distance) % 4)


def table_kernel(
    box, merge_hbm, spread_hbm,
    ec, es, switch, rc, rs, merge, spread,
    first, second, left, right, sems,
):
    group = lax.axis_index("grp")
    device = lax.axis_index("dev")
    copies = [
        pltpu.make_async_copy(merge_hbm, merge, sems.at[0]),
        pltpu.make_async_copy(spread_hbm.at[group], spread, sems.at[1]),
    ]
    for copy in copies:
        copy.start()
    z = device % 4
    lane = lanes()
    node = by_sublane(Z)
    u1x, u1y = group % 2, group // 2
    u2 = lane // 32
    u2x, u2y = u2 % 2, u2 // 2

    space, wave = box[0], box[1]
    space_x, space_y = space // 32, space % 32
    wave_x, wave_y = wave // 16, wave % 16

    for u0 in range(4):
        ix, iy = 2 * space_x + u0 % 2, 2 * space_y + u0 // 2
        fx, fy = ix.astype(F32) + 0.5, iy.astype(F32) + 0.5
        one, two = speeds(cos_sin(fx * 0.125), cos_sin(fy * 0.125))
        for c in range(4):
            kx = wave_x * 8 + u2x * 4 + u1x * 2 + c % 2 - 64
            ky = wave_y * 8 + u2y * 4 + u1y * 2 + c // 2 - 64
            whole = (((2 * ix + 1) * kx + (2 * iy + 1) * ky) & 3).astype(F32) * 0.25
            fkx, fky = kx.astype(F32), ky.astype(F32)
            k2 = (fky + node) * 32.0
            part2 = whole + fy * 0.5 * node
            rad2 = two * (k2 * k2)
            for s1 in range(8):
                k1 = (fkx + Z[s1]) * 32.0
                turns = part2 + fx * (0.5 * Z[s1]) + root(one * (k1 * k1) + rad2)
                cosine, sine = cos_sin(turns)
                ec[u0, c, pl.ds(8 * s1, 8), :] = cosine
                es[u0, c, pl.ds(8 * s1, 8), :] = -sine

    u0 = lane // 8 % 4
    ix, iy = 2 * space_x + u0 % 2, 2 * space_y + u0 // 2
    kx, ky = wave_x * 4 + u2x * 2 + u1x - 32, wave_y * 4 + u2y * 2 + u1y - 32
    fx, fy = ix.astype(F32), iy.astype(F32)
    fkx, fky = kx.astype(F32), ky.astype(F32)
    half_x = ((kx + ix) & 1).astype(F32) * 0.5
    half_y = ((ky + iy) & 1).astype(F32) * 0.5
    one_a, two_a = speeds(cos_sin((fx + 0.5) * 0.125), cos_sin((fy + 0.5) * 0.125))
    turn2 = cos_sin((fy + node) * 0.125)
    squares1, squares2 = [], []
    for s in range(8):
        k1, k2 = (fkx + Z[s]) * 64.0, (fky + Z[s]) * 64.0
        squares1.append(k1 * k1)
        squares2.append(k2 * k2)
    for s1 in range(8):
        for s2 in range(8):
            linear = (2.0 * fy + 0.5) * Z[s2] + node * (Z[s2] - 0.5) + half_y
            right[s1, s2] = fraction(linear + root(one_a * squares1[s1] + two_a * squares2[s2]))
    b1, b2 = (fkx + 0.5) * 64.0, (fky + 0.5) * 64.0
    for t1 in range(8):
        one, two = speeds(cos_sin((fx + Z[t1]) * 0.125), turn2)
        back = root(one * (b1 * b1) + two * (b2 * b2))
        for s in range(8):
            linear = (2.0 * fx + 0.5) * Z[s] + (Z[t1] * (Z[s] - 0.5)) + half_x
            left[t1, s] = fraction(linear - back)
            first[t1, s] = one * squares1[s]
            second[t1, s] = two * squares2[s]

    def switch_rows(s1, _):
        for s2 in range(8):
            cosines, sines = [], []
            for t1 in range(8):
                turns = left[t1, s1] + right[s1, s2] + root(first[t1, s1] + second[t1, s2])
                cosine, sine = cos_sin(turns, 1.0 / 64.0)
                cosines.append(cosine)
                sines.append(sine)
            turned = jnp.concatenate(cosines + sines).T
            for tile in range(16):
                switch[pl.ds(tile * 8 * PITCH + s1 * 8 + s2, 8, stride=PITCH), :] = turned[8 * tile : 8 * tile + 8]
        return 0

    lax.fori_loop(0, 8, switch_rows, 0)

    space, wave = box[2], box[3]
    ix, iy = space // 32, space % 32
    for bit_x, bit_y in ((z % 2, z // 2), (u1x, u1y), (u2x, u2y)):
        ix, iy = 2 * ix + bit_x, 2 * iy + bit_y
    fx, fy = ix.astype(F32), iy.astype(F32)
    fkx = (wave // 16 - 8).astype(F32) + 0.5
    fky = (wave % 16 - 8).astype(F32) + 0.5
    halves = ((ix + iy) & 1).astype(F32) * 0.5
    turn2 = cos_sin((fy + node) * 0.03125)
    b1, b2 = fkx * 256.0, fky * 256.0
    for t1 in range(8):
        one, two = speeds(cos_sin((fx + Z[t1]) * 0.03125), turn2)
        turns = halves + fkx * Z[t1] + fky * node + root(one * (b1 * b1) + two * (b2 * b2))
        cosine, sine = cos_sin(turns)
        rc[pl.ds(8 * t1, 8), :] = cosine
        rs[pl.ds(8 * t1, 8), :] = sine
    for copy in copies:
        copy.wait()


def split(value):
    high = value.astype(BF16)
    return high, (value - high.astype(F32)).astype(BF16)


def dot(a, b):
    return jnp.dot(a, b, preferred_element_type=F32)


def main_kernel(y0, y1, y2, y3, ec, es, switch, merge, out, turned_high, turned_low, turned, sums):
    z = lax.axis_index("dev") % 4
    for u0 in range(4):
        for distance, y in zip(ORDER, (y0, y1, y2, y3)):
            child = (z + 4 - distance) % 4
            start = pl.multiple_of(child * 64, 64)
            for half in range(4):
                spot = pl.ds(16 * half, 16)
                cosine, sine = ec[u0, child, spot, :], es[u0, child, spot, :]
                for low in range(2):
                    re, im = y[0, low, spot, :], y[1, low, spot, :]
                    for part, value in enumerate((re * cosine - im * sine, re * sine + im * cosine)):
                        high, rest = split(value)
                        columns = pl.ds((2 * part + low) * 128, 128)
                        turned_high[pl.ds(start + 16 * half, 16), columns] = high
                        turned_low[pl.ds(start + 16 * half, 16), columns] = rest
        product = dot(merge[...], turned_high[...])
        summed = product[:64] + product[64:] + dot(merge[:64], turned_low[...])
        for low in range(2):
            re, im = summed[:, low * 128 : low * 128 + 128], summed[:, (2 + low) * 128 : (2 + low) * 128 + 128]
            flat = jnp.concatenate([re, im]).T
            for u2 in range(4):
                for high in range(4):
                    start = (u2 * 32 + u0 * 8) * 8 + low * 4 + high
                    tile = (u2 * 4 + high) * 8
                    turned[pl.ds(start, 8, stride=8), :] = flat[tile : tile + 8]

    lane = lanes()
    left = lane < 64
    for u0 in range(4):
        for r in range(8):
            pair = [u2 * 32 + u0 * 8 + r for u2 in range(4)]
            value = [turned[pl.ds(8 * m, 8), :] for m in pair]
            other = [pltpu.roll(v, 64, 1) for v in value]
            re = [jnp.where(left, value[u], other[u + 1]) for u in (0, 2)]
            im = [jnp.where(left, other[u], value[u + 1]) for u in (0, 2)]
            high, low = split(jnp.concatenate([jnp.concatenate(re, axis=1), jnp.concatenate(im, axis=1)]))
            matrix_high, matrix_low = split(jnp.concatenate([switch[pl.ds(PITCH * m, 64), :] for m in pair]))
            product = dot(jnp.concatenate([high, low]), matrix_high)
            product = product[:16] + product[16:] + dot(high, matrix_low)
            crossed = pltpu.roll(product[8:], 64, 1)
            total = product[:8] + jnp.where(left, -crossed, crossed)
            sums[u0, pl.ds(r, 8, stride=8), :] = total
            sums[u0, pl.ds(64 + r, 8, stride=8), :] = pltpu.roll(total, 64, 1)
    for u0 in range(4):
        out[u0] = sums[u0].T[:64]


def sum_kernel(own, other, out0, out1, out2, out3):
    z = lax.axis_index("dev") % 4
    for distance, out in zip(BACK, (out0, out1, out2, out3)):
        target = (z + distance) % 4
        out[...] = own[target] + other[target]


def last_kernel(r0, r1, r2, r3, spread, rc, rs, target, held, high_ref, low_ref, spreaded, out, sems):
    z = lax.axis_index("dev") % 4
    for distance, r in zip(BACK, (r0, r1, r2, r3)):
        held[(z + 4 - distance) % 4] = r[...]
    for tile in range(4):
        spot = pl.ds(16 * tile, 16)
        for low, value in enumerate(swap_four([held[source, spot, :] for source in range(4)], 8)):
            high, rest = split(value)
            high_ref[low, spot, :] = high
            low_ref[low, spot, :] = rest
    for low in range(4):
        spreaded[low] = (
            dot(spread[0], high_ref[low]) + dot(spread[0], low_ref[low]) + dot(spread[1], high_ref[low])
        )
    copies = []
    for tile in range(8):
        entry = [None] * 16
        for low in range(4):
            parts = [spreaded[low, pl.ds(64 * u2 + 8 * tile, 8), :] for u2 in range(4)]
            for high, value in enumerate(swap_wide(parts)):
                entry[4 * high + low] = value
        spot = pl.ds(8 * tile, 8)
        cosine, sine = rc[spot, :], rs[spot, :]
        for k in range(8):
            re, im = entry[k], entry[8 + k]
            out[0, k, spot, :] = re * cosine - im * sine
            out[1, k, spot, :] = re * sine + im * cosine
        if tile % 2:
            rows = pl.ds(8 * tile - 8, 16)
            copies.append(pltpu.make_async_copy(out.at[:, :, rows, :], target.at[:, :, rows, :], sems.at[tile // 2]))
            copies[-1].start()
    for copy in copies:
        copy.wait()


def call(kernel, inputs, outs, scratch=(), flops=0, place=VMEM):
    return pl.pallas_call(
        kernel,
        out_shape=outs,
        in_specs=[spec for spec, _ in inputs],
        out_specs=jax.tree.map(lambda _: place, outs),
        scratch_shapes=scratch,
        cost_estimate=pl.CostEstimate(flops=flops, bytes_accessed=1 << 20, transcendentals=0),
        compiler_params=pltpu.CompilerParams(vmem_limit_bytes=40 << 20),
    )(*[value for _, value in inputs])


def in_hbm(value):
    return pltpu.with_memory_space_constraint(value, pltpu.HBM)


def shape(*dims, kind=F32):
    return jax.ShapeDtypeStruct(dims, kind)


def along_z(value, distance):
    route = [(low, low // 4 * 4 + (low + distance) % 4) for low in range(lax.axis_size("dev"))]
    return lax.ppermute(value, "dev", route)


def across_groups(value, bit):
    return lax.ppermute(value, "grp", [(low, low ^ bit) for low in range(4)])


def per_device(coefficients, spatial_root, frequency_root):
    far, held, box = call(
        pack_far_kernel,
        [(HBM, in_hbm(value)) for value in (coefficients, spatial_root, frequency_root)],
        [shape(2, 2, 64, 128), shape(2, 8, 64, 128), shape(4, 8, 128, kind=jnp.int32)],
        [pltpu.SMEM((256,), jnp.int32)] * 2 + [pltpu.SemaphoreType.DMA((6,))],
        flops=1 << 20,
    )
    arrived = [along_z(far, ORDER[0])]
    near = call(pack_near_kernel, [(VMEM, held)], [shape(2, 2, 64, 128)] * 3, flops=1 << 20)
    arrived += [along_z(near[0], ORDER[1]), along_z(near[1], ORDER[2]), near[2]]
    tables = call(
        table_kernel,
        [(VMEM, box), (HBM, in_hbm(in_two(MERGE).reshape(128, 256))), (HBM, in_hbm(in_two(SPREAD, 1)))],
        [shape(4, 4, 64, 128)] * 2
        + [shape(128 * PITCH, 128)]
        + [shape(64, 128)] * 2
        + [shape(128, 256, kind=BF16), shape(2, 256, 64, kind=BF16)],
        [pltpu.VMEM((8, 8, 8, 128), F32)] * 4 + [pltpu.SemaphoreType.DMA((2,))],
        flops=1 << 26,
    )
    ec, es, switch, rc, rs, merge, spread = tables
    partial = call(
        main_kernel,
        [(VMEM, value) for value in (*arrived, ec, es, switch, merge)],
        shape(4, 64, 128),
        [
            pltpu.VMEM((256, 512), BF16),
            pltpu.VMEM((256, 512), BF16),
            pltpu.VMEM((1024, 128), F32),
            pltpu.VMEM((4, 128, 128), F32),
        ],
        flops=1 << 27,
    )
    partial = partial + across_groups(partial, 1)
    summed = call(
        sum_kernel,
        [(VMEM, partial), (VMEM, across_groups(partial, 2))],
        [shape(64, 128)] * 4,
        flops=1 << 18,
    )
    blocks = [along_z(piece, distance) if distance else piece for distance, piece in zip(BACK, summed)]
    return call(
        last_kernel,
        [(VMEM, value) for value in (*blocks, spread, rc, rs)],
        shape(2, 8, 64, 128),
        [
            pltpu.VMEM((4, 64, 128), F32),
            pltpu.VMEM((4, 64, 128), BF16),
            pltpu.VMEM((4, 64, 128), BF16),
            pltpu.VMEM((4, 256, 128), F32),
            pltpu.VMEM((2, 8, 64, 128), F32),
            pltpu.SemaphoreType.DMA((4,)),
        ],
        flops=1 << 24,
        place=HBM,
    )


def solution(mesh):
    return jax.shard_map(
        per_device,
        mesh=mesh,
        in_specs=(P(None, None, None, ("grp", "dev")), P(), P()),
        out_specs=P(None, None, None, ("grp", "dev")),
        check_vma=False,
    )
```
